128 devices in a mesh: px: 16 (over y, z), py: 8 (over x, core).
Axes of the slice: x: 4, y: 4, z: 4, core: 2. Of those that a mesh axis runs over, the one named last changes fastest.
Arguments:
- initial_field: float32 [1, 2048, 2048], P(None, ('px', 'py')), may hold values from -6 to 6
- target_field: float32 [1, 2048, 2048], P(None, ('px', 'py')), may hold values from -6 to 6
- forcing: float32 [2, 2048, 2048], P(None, ('px', 'py')), may hold values from -6 to 6
Outputs:
- next_field: float32 [1, 2048, 2048], P(None, ('px', 'py'))
- objective: float32 [], replicated
- field_grad: float32 [1, 2048, 2048], P(None, ('px', 'py'))
- forcing_grad: float32 [2, 2048, 2048], P(None, ('px', 'py'))
The draws below stay inside these ranges and needn't reach their ends.
All inputs are finite; a program needn't handle non-finite values.
Results may differ from the reference program's by a relative error of at most 0.00014.
Values sent between devices are 32-bit elements; how exact they have to be, the bound alone decides.
A program may use at most 64 MiB of HBM per device.

```python
import jax
import jax.numpy as jnp
from jax import lax

NX = 2048
NY = 2048
MEMBERS = 1


def block_scale(own_key, dims, shards, low, largest):
    def one(dim, shards_of):
        heights = jax.random.uniform(jax.random.fold_in(jax.random.fold_in(own_key, 6), dim), (shards_of,), jnp.float32, low / len(shards), largest / len(shards))
        return jnp.repeat(jnp.exp(heights), dims[dim] // shards_of).reshape((-1,) + (1,) * (len(dims) - dim - 1))

    level = one(*shards[0])
    for cut in shards[1:]:
        level = level * one(*cut)
    return level


def gaussian(key, extent, deviation, bound, cuts=(), held_as=jnp.bfloat16):
    values = deviation * jax.random.normal(key, extent, jnp.float32)
    if cuts:
        values = values * block_scale(key, extent, cuts, -0.22, 0.18)
    return jnp.clip(values, -bound, bound).astype(held_as)


def setup_inputs(seed: int = 0) -> dict:
    arg_keys = jax.random.split(jax.random.key(seed), 4)
    initial_field = gaussian(arg_keys[0], (MEMBERS, NX, NY), 1.0, 6.0, ((1, 128),), jnp.float32)
    target_field = gaussian(arg_keys[1], (MEMBERS, NX, NY), 1.0, 6.0, ((1, 128),), jnp.float32)
    forcing = gaussian(arg_keys[2], (2, NY, NX), 1.0, 6.0, ((1, 128),), jnp.float32)
    return {"initial_field": initial_field, "target_field": target_field, "forcing": forcing}


time_step = 0.25

def wavenumbers(count):
    position = jnp.arange(count, dtype=jnp.int32)
    signed = jnp.where(position < count // 2, position, position - count)
    waves = (4.0 * signed.astype(jnp.float32) / count).astype(jnp.float32)
    derive = jnp.where(position == count // 2, jnp.float32(0.0), waves).astype(jnp.float32)
    return (waves, derive)

def advance(field, forcing):
    wave_first, deriv_first = wavenumbers(NX)
    wave_second, deriv_second = wavenumbers(NY)
    wave_square = wave_first[:, None] ** 2 + wave_second[None, :] ** 2
    denominator = 1.0 + time_step * (wave_square * wave_square - wave_square)
    state_hat = jnp.fft.fft2(field, norm='ortho')
    grad_first = jnp.fft.ifft2(1j * deriv_first[:, None] * state_hat, norm='ortho').real
    grad_second = jnp.fft.ifft2(1j * deriv_second[None, :] * state_hat, norm='ortho').real
    nonlinear = -0.5 * (grad_first * grad_first + grad_second * grad_second)
    nonlinear_hat = jnp.fft.fft2(nonlinear, norm='ortho')
    forcing_hat = lax.complex(forcing[0].T, forcing[1].T)
    next_hat = (state_hat + time_step * (nonlinear_hat + forcing_hat)) / denominator
    return jnp.fft.ifft2(next_hat, norm='ortho').real

def reference(initial_field, target_field, forcing):

    def one_member(pair):
        field, goal = pair
        next_one, pullback = jax.vjp(advance, field, forcing)
        residual = next_one - goal
        grad_one, forcing_one = pullback(residual)
        return (next_one, jnp.sum(residual * residual), grad_one, forcing_one)
    next_field, squares, field_grad, forcing_parts = lax.map(one_member, (initial_field, target_field))
    objective = 0.5 * jnp.sum(squares) / (MEMBERS * NX * NY)
    forcing_grad = lax.optimization_barrier(jnp.sum(forcing_parts, axis=0))
    return (next_field, objective, field_grad, forcing_grad)
```

```python
import math

import jax
import jax.numpy as jnp
from jax import lax
from jax.experimental import pallas as pl
from jax.experimental.pallas import tpu as pltpu
from jax.sharding import PartitionSpec as P

PX_PY = ("px", "py")
PX = "px"
PY = "py"


time_step = 0.25
highest = lax.Precision.HIGHEST


def in_blocks(shard, dim, length):
    dims = shard.shape
    tiles = shard.reshape(*dims[:dim], length, dims[dim] // length, *dims[dim + 1 :])
    return jnp.moveaxis(tiles, dim, 0)


def laid_out(tiles, dim):
    tiles = jnp.moveaxis(tiles, 0, dim)
    dims = tiles.shape
    return tiles.reshape(*dims[:dim], dims[dim] * dims[dim + 1], *dims[dim + 2 :])


MESH = pl.DeviceIdType.MESH
peers = 128


def swap_kernel(x_ref, o_ref, recv, send_sem, recv_sem, own_sem):
    me = lax.axis_index("px") * 8 + lax.axis_index("py")
    barrier = pltpu.get_barrier_semaphore()

    def greet(i, carry):
        d = jnp.bitwise_xor(me, i)
        pl.semaphore_signal(barrier, inc=1, device_id=(d // 8, d % 8), device_id_type=MESH)
        return carry

    lax.fori_loop(1, peers, greet, 0)
    pl.semaphore_wait(barrier, peers - 1)
    own = pltpu.make_async_copy(x_ref.at[me], recv.at[me], own_sem)
    own.start()

    def send(i, carry):
        d = jnp.bitwise_xor(me, peers - i)
        pltpu.make_async_remote_copy(
            x_ref.at[d], recv.at[me], send_sem, recv_sem,
            device_id=(d // 8, d % 8), device_id_type=MESH,
        ).start()
        return carry

    lax.fori_loop(1, peers, send, 0)
    own.wait()
    whole = pltpu.make_async_remote_copy(
        x_ref.at[pl.ds(0, peers - 1)], recv.at[pl.ds(0, peers - 1)], send_sem, recv_sem,
        device_id=(0, 0), device_id_type=MESH,
    )
    whole.wait_recv()
    whole.wait_send()
    o_ref[...] = recv[...]


def swap(x):
    shape = (peers, 2, 128)
    return pl.pallas_call(
        swap_kernel,
        out_shape=jax.ShapeDtypeStruct(shape, jnp.float32),
        in_specs=[pl.BlockSpec(memory_space=pltpu.VMEM)],
        out_specs=pl.BlockSpec(memory_space=pltpu.VMEM),
        scratch_shapes=[
            pltpu.VMEM(shape, jnp.float32),
            pltpu.SemaphoreType.DMA,
            pltpu.SemaphoreType.DMA,
            pltpu.SemaphoreType.DMA,
        ],
        compiler_params=pltpu.CompilerParams(collective_id=0, has_side_effects=True),
    )(x)


def one_exchange(shard, axis, axes, splits, concats):
    sizes = [lax.axis_size(a) for a in axes]
    tiles = in_blocks(shard, splits[0], sizes[0])
    tiles = jnp.moveaxis(in_blocks(tiles, splits[1] + 1, sizes[1]), 0, 1)
    inside = tiles.shape[2:]
    tiles = tiles.reshape(-1, *inside)
    tiles = swap(tiles.reshape(128, 2, 128)).reshape(tiles.shape)
    tiles = laid_out(tiles.reshape(*sizes, *inside), concats[0] + 1)
    return laid_out(tiles, concats[1])


def one_axis_at_a_time(shard, axes):
    for axis in axes:
        shard = lax.psum(shard, axis)
    return shard


def factor_pair(length):
    first_len = int(math.isqrt(length))
    while length % first_len:
        first_len -= 1
    return (first_len, length // first_len)


def phases(row_count, col_count, period, sign_value, factor):
    product = (
        jnp.arange(row_count, dtype=jnp.int32)[:, None]
        * jnp.arange(col_count, dtype=jnp.int32)[None, :]
        % period
    )
    angles = product.astype(jnp.float32) * (2.0 * math.pi / period)
    return (factor * jnp.cos(angles), sign_value * factor * jnp.sin(angles))


def complex_einsum(formula, left_real, left_imag, table_pair):
    real_term = jnp.einsum(formula, left_real, table_pair[0], precision=highest)
    imag_term = jnp.einsum(formula, left_real, table_pair[1], precision=highest)
    if left_imag is None:
        return (real_term, imag_term)
    real_term = real_term - jnp.einsum(formula, left_imag, table_pair[1], precision=highest)
    imag_term = imag_term + jnp.einsum(formula, left_imag, table_pair[0], precision=highest)
    return (real_term, imag_term)


def transform(real_part, imag_part, sign_value, leading, real_only):
    if leading:
        members, length, span_rows = real_part.shape
        first_len, second_len = factor_pair(length)
        new_shape = (members, first_len, second_len, span_rows)
        formula = "mabr,ak->mrkb"
    else:
        members, span_rows, length = real_part.shape
        first_len, second_len = factor_pair(length)
        new_shape = (members, span_rows, first_len, second_len)
        formula = "mrab,ak->mrkb"
    shaped_real = real_part.reshape(new_shape)
    shaped_imag = None if imag_part is None else imag_part.reshape(new_shape)
    sectioned_out = complex_einsum(
        formula, shaped_real, shaped_imag, phases(first_len, first_len, first_len, sign_value, 1.0)
    )
    twiddle = phases(first_len, second_len, length, sign_value, 1.0 / math.sqrt(length))
    turned_real = sectioned_out[0] * twiddle[0] - sectioned_out[1] * twiddle[1]
    turned_imag = sectioned_out[0] * twiddle[1] + sectioned_out[1] * twiddle[0]
    last_table = phases(second_len, second_len, second_len, sign_value, 1.0)
    final_formula = "mrkb,bq->mrqk"
    if real_only:
        out_real = jnp.einsum(final_formula, turned_real, last_table[0], precision=highest)
        out_real = out_real - jnp.einsum(
            final_formula, turned_imag, last_table[1], precision=highest
        )
        return (out_real.reshape(members, span_rows, length), None)
    out_real, out_imag = complex_einsum(final_formula, turned_real, turned_imag, last_table)
    return (
        out_real.reshape(members, span_rows, length),
        out_imag.reshape(members, span_rows, length),
    )


def reorder(block, outer_count, inner_count):
    members, full_len, span_cols = block.shape
    blocks = block.reshape(
        members, inner_count, outer_count, full_len // (outer_count * inner_count), span_cols
    )
    return jnp.swapaxes(blocks, 1, 2).reshape(members, full_len, span_cols)


def regroup(real_part, imag_part):
    moved_real, moved_imag = (
        one_exchange(real_part, PX_PY, (PX, PY), (2, 2), (1, 1)),
        one_exchange(imag_part, PX_PY, (PX, PY), (2, 2), (1, 1)),
    )
    outer_count = lax.axis_size(PX)
    inner_count = lax.axis_size(PY)
    moved_real = reorder(moved_real, outer_count, inner_count)
    moved_imag = reorder(moved_imag, outer_count, inner_count)
    return (moved_real, moved_imag)


def spectral(real_part, imag_part):
    first_pass = transform(real_part, imag_part, -1.0, False, False)
    moved = regroup(first_pass[0], first_pass[1])
    return transform(moved[0], moved[1], -1.0, True, False)


def physical(real_part, imag_part, real_only):
    first_pass = transform(real_part, imag_part, 1.0, False, False)
    moved = regroup(first_pass[0], first_pass[1])
    return transform(moved[0], moved[1], 1.0, True, real_only)


def waves_of(position, count):
    signed = jnp.where(position < count // 2, position, position - count)
    waves = 4.0 * signed.astype(jnp.float32) / count
    derive = jnp.where(position == count // 2, jnp.float32(0.0), waves)
    return (waves, derive)


def per_device(initial_field, target_field, forcing):
    members = initial_field.shape[0]
    full_second = initial_field.shape[2]
    spec_rows = forcing.shape[1]
    full_first = forcing.shape[2]
    device = lax.axis_index(PX_PY)
    position_first = jnp.arange(full_first, dtype=jnp.int32)
    position_second = device * spec_rows + jnp.arange(spec_rows, dtype=jnp.int32)
    wave_first, deriv_first = waves_of(position_first, full_first)
    wave_second, deriv_second = waves_of(position_second, full_second)
    wave_first = wave_first[None, :]
    deriv_first = deriv_first[None, :]
    wave_second = wave_second[:, None]
    deriv_second = deriv_second[:, None]
    wave_square = wave_first * wave_first + wave_second * wave_second
    denominator = 1.0 + time_step * (wave_square * wave_square - wave_square)
    state_real, state_imag = spectral(initial_field, None)
    slope_real = -deriv_first * state_imag - deriv_second * state_real
    slope_imag = deriv_first * state_real - deriv_second * state_imag
    grad_first, grad_second = physical(slope_real, slope_imag, False)
    nonlinear = -0.5 * (grad_first * grad_first + grad_second * grad_second)
    nonlinear_real, nonlinear_imag = spectral(nonlinear, None)
    next_real = (state_real + time_step * (nonlinear_real + forcing[0])) / denominator
    next_imag = (state_imag + time_step * (nonlinear_imag + forcing[1])) / denominator
    next_field, unused_part = physical(next_real, next_imag, True)
    residual = next_field - target_field
    total = one_axis_at_a_time(0.5 * jnp.sum(residual * residual), PX_PY)
    objective = total / (members * full_first * full_second)
    misfit_real, misfit_imag = spectral(residual, None)
    coef_real = misfit_real / denominator
    coef_imag = misfit_imag / denominator
    forcing_grad = time_step * jnp.stack([jnp.sum(coef_real, axis=0), jnp.sum(coef_imag, axis=0)])
    multiplier, unused_other = physical(time_step * coef_real, time_step * coef_imag, True)
    joint_real, joint_imag = spectral(multiplier * grad_first, multiplier * grad_second)
    total_real = coef_real - deriv_first * joint_imag + deriv_second * joint_real
    total_imag = coef_imag + deriv_first * joint_real + deriv_second * joint_imag
    field_grad, unused_last = physical(total_real, total_imag, True)
    return (next_field, objective, field_grad, forcing_grad)


def solution(mesh):
    in_specs = (P(None, PX_PY, None), P(None, PX_PY, None), P(None, PX_PY, None))
    out_specs = (P(None, PX_PY, None), P(), P(None, PX_PY, None), P(None, PX_PY, None))
    return jax.shard_map(
        per_device, mesh=mesh, in_specs=in_specs, out_specs=out_specs, check_vma=False
    )
```

```python
import math

import jax
import jax.numpy as jnp
import numpy as np
from jax import lax
from jax.experimental import pallas as pl
from jax.experimental.pallas import tpu as pltpu
from jax.sharding import PartitionSpec as P

MESH = pl.DeviceIdType.MESH
f32 = jnp.float32
bf16 = jnp.bfloat16

n = 2048
peers = 128
step = 0.25
unit = 4.0 / n
half_rows = 72


def cplx(table):
    return np.block([[table.real, table.imag], [-table.imag, table.real]])


def signed(count, index):
    return np.where(index < count // 2, index, index - count)


def build_tables():
    s = np.arange(128)
    a1 = np.arange(65)
    theta = 2 * np.pi * np.outer(a1, s) / 128
    td = np.zeros((2 * half_rows, 128))
    td[:65] = np.cos(theta)
    td[half_rows : half_rows + 65] = -np.sin(theta)
    weight = np.where((a1 == 0) | (a1 == 64), 1.0, 2.0) / 128
    ti = np.zeros((128, 2 * half_rows))
    ti[:, :65] = (np.cos(theta) * weight[:, None]).T
    ti[:, half_rows : half_rows + 65] = (-np.sin(theta) * weight[:, None]).T

    def derivative(length, factor):
        freq = signed(length, s[:length]).astype(float) * factor
        inner = np.where(s[:length] == length // 2, 0.0, freq)
        gap = np.subtract.outer(s[:length], s[:length])
        waves = np.exp(2j * np.pi * gap[:, :, None] * s[:length] / length)
        smooth = (waves * (1j * inner)).sum(-1).real / length
        nyquist = freq[length // 2] * (-1.0) ** gap / length
        return (smooth + 1j * nyquist).T

    root = 1.0 / math.sqrt(n)
    mx = cplx(np.kron(np.eye(8), derivative(16, unit * 128)))
    my = cplx(derivative(128, unit * 16) / 16)

    w16 = np.exp(-2j * np.pi * np.outer(s[:16], s[:16]) / 16)
    eye8 = np.eye(8)
    forward = w16.reshape(16, 2, 8)
    parts = np.zeros((2, 8, 16, 2, 2, 8, 8))
    for y in range(8):
        parts[0, y, :, :, 0, :, y] = forward.real
        parts[0, y, :, :, 1, :, y] = forward.imag
        parts[1, y, :, :, 0, :, y] = -forward.imag
        parts[1, y, :, :, 1, :, y] = forward.real
    wx = parts.reshape(256, 256) * root
    back = w16.conj().T.reshape(2, 8, 16)
    parts = np.zeros((2, 2, 8, 8, 2, 8, 16))
    for y in range(8):
        parts[:, 0, :, y, 0, y, :] = back.real
        parts[:, 0, :, y, 1, y, :] = back.imag
        parts[:, 1, :, y, 0, y, :] = -back.imag
        parts[:, 1, :, y, 1, y, :] = back.real
    wxi = parts.reshape(256, 256) * (128 * root)
    forward = w16.reshape(2, 8, 16)
    parts = np.zeros((2, 2, 8, 8, 2, 2, 8, 16))
    for k in range(8):
        for c in range(2):
            parts[:, c, k, :, c, 0, k, :] = forward.real
            parts[:, c, k, :, c, 1, k, :] = forward.imag
    wy = parts.reshape(256, 512)
    back = w16.conj().T.reshape(16, 2, 8)
    parts = np.zeros((2, 8, 16, 2, 2, 8, 8))
    for k in range(8):
        parts[0, k, :, :, 0, k, :] = back.real
        parts[0, k, :, :, 1, k, :] = back.imag
        parts[1, k, :, :, 0, k, :] = -back.imag
        parts[1, k, :, :, 1, k, :] = back.real
    wyi = parts.reshape(256, 256)
    f128 = np.exp(-2j * np.pi * np.outer(s, s) / 128) * root
    ty = cplx(f128).T
    tyi = cplx(f128.conj()).T
    squares = np.stack([mx, my, wx, wxi, wy[:, :256], wy[:, 256:], wyi, ty, tyi])

    own = np.zeros((128, 2, 128))
    mirror = np.zeros((128, 2, 128))
    for e in range(128):
        h, a = e % 2, e // 2
        if e == 0:
            own[e, 0, 0] = mirror[e, 1, 0] = 1
        elif e == 1:
            own[e, 0, 64] = mirror[e, 1, 64] = 1
        else:
            own[e, h, a] = mirror[e, 1 - h, 128 - a] = 1
    places = np.stack([own.reshape(128, 256), mirror.reshape(128, 256)])

    row = np.arange(half_rows)[:, None]
    lane = np.arange(128)[None, :]
    twx = 2 * np.pi * row * (lane % 16) / n
    twy = 2 * np.pi * np.arange(128)[:, None] * (lane % 16) / n
    twr = 2 * np.pi * np.arange(16)[:, None] * lane / n
    both = lambda t: np.stack([np.cos(t), np.sin(t)]).astype(np.float32)

    def halves(t):
        high = t.astype(np.float32).astype(bf16)
        low = (t - high.astype(np.float64)).astype(np.float32).astype(bf16)
        return high, low

    return dict(
        squares=np.stack(halves(squares), axis=1),
        td=np.stack(halves(td)),
        ti=np.stack(halves(ti)),
        places=places.astype(np.float32).astype(bf16),
        places_t=places.transpose(0, 2, 1).astype(np.float32).astype(bf16),
        twx=both(twx),
        twy=both(twy),
        twr=both(twr),
    )


MX, MY, WX, WXI, WYA, WYB, WYI, TY, TYI = range(9)
NAMES = ("squares", "td", "ti", "places", "places_t", "twx", "twy", "twr")


def split(x):
    high = x.astype(bf16)
    return high, (x - high.astype(f32)).astype(bf16)


def dot(a, b):
    return jnp.dot(a, b, preferred_element_type=f32)


def product(a, b):
    return dot(a[0], b[0]) + (dot(a[0], b[1]) + dot(a[1], b[0]))


def left(table, x):
    return product((table[0], table[1]), split(x))


def right(x, table):
    return product(split(x), (table[0], table[1]))


def cat(parts, axis):
    return jnp.concatenate(parts, axis=axis)


def turn(re, im, cos, sin):
    return re * cos + im * sin, im * cos - re * sin


def turn_back(re, im, cos, sin):
    return re * cos - im * sin, im * cos + re * sin


def real_dft(values):
    count = len(values)
    if count == 2:
        return [(values[0] + values[1], None), (values[0] - values[1], None)]
    even, odd = real_dft(values[0::2]), real_dft(values[1::2])
    quarter = count // 4
    out = [None] * (count // 2 + 1)
    for k in range(quarter + 1):
        (er, ei), (tr, ti) = even[k], odd[k]
        if k == quarter:
            out[k] = (er, -tr)
            continue
        if k > 0:
            c, s = math.cos(2 * math.pi * k / count), math.sin(2 * math.pi * k / count)
            tr, ti = (tr * c + ti * s, ti * c - tr * s) if ti is not None else (tr * c, tr * -s)
        if k == 0:
            out[0], out[count // 2] = (er + tr, None), (er - tr, None)
        else:
            ei = 0.0 if ei is None else ei
            out[k] = (er + tr, ei + ti)
            out[count // 2 - k] = (er - tr, ti - ei)
    return out


def real_idft(spectrum):
    count = 2 * (len(spectrum) - 1)
    if count == 2:
        return [spectrum[0][0] + spectrum[1][0], spectrum[0][0] - spectrum[1][0]]
    quarter = count // 4
    even, odd = [], []
    for k in range(quarter + 1):
        re, im = spectrum[k]
        if k == 0:
            other = spectrum[count // 2][0]
            even.append((re + other, None))
            odd.append((re - other, None))
        elif k == quarter:
            even.append((2.0 * re, None))
            odd.append((-2.0 * im, None))
        else:
            hr, hi = spectrum[count // 2 - k]
            even.append((re + hr, im - hi))
            dr, di = re - hr, im + hi
            c, s = math.cos(2 * math.pi * k / count), math.sin(2 * math.pi * k / count)
            odd.append((dr * c - di * s, dr * s + di * c))
    xs, ys = real_idft(even), real_idft(odd)
    return [v for pair in zip(xs, ys) for v in pair]


def rows_derivative(tiles, t):
    cos, sin = t["twr"][0], t["twr"][1]
    turned = []
    for k, (re, im) in enumerate(real_dft(tiles)):
        c, s = cos[k : k + 1], sin[k : k + 1]
        if k == 0:
            turned.append((re, jnp.zeros_like(re)))
        elif im is None:
            turned.append((re * c, -re * s))
        else:
            turned.append(turn(re, im, c, s))
    re_rows = cat([v[0] for v in turned], 0)
    im_rows = cat([v[1] for v in turned], 0)
    moved = right(cat([re_rows, im_rows], 1), t["squares"][MY])
    out = []
    for k, (re, im) in enumerate(turned):
        mr = moved[16 * k : 16 * k + 16, :128] - (unit / 16 * k) * im
        mi = moved[16 * k : 16 * k + 16, 128:] + (unit / 16 * k) * re
        out.append(turn_back(mr, mi, cos[k : k + 1], sin[k : k + 1]))
    return real_idft(out)


def columns_half(x, t):
    y = left(t["td"], x)
    cos, sin = t["twx"][0], t["twx"][1]
    out = []
    for g in range(x.shape[1] // 128):
        part = y[:, 128 * g : 128 * g + 128]
        out.append(turn(part[:half_rows], part[half_rows:], cos, sin))
    return out


def columns_back(parts, t):
    cos, sin = t["twx"][0], t["twx"][1]
    cols = []
    for re, im in parts:
        br, bi = turn_back(re, im, cos, sin)
        cols.append(cat([br, bi], 0))
    return left(t["ti"], cat(cols, 1))


def columns_derivative(x, t):
    parts = columns_half(x, t)
    stacked = cat([cat([re, im], 1) for re, im in parts], 0)
    moved = right(stacked, t["squares"][MX])
    slope = unit * lax.broadcasted_iota(jnp.int32, (half_rows, 128), 0).astype(f32)
    out = []
    for g, (re, im) in enumerate(parts):
        rows = slice(half_rows * g, half_rows * (g + 1))
        out.append((moved[rows, :128] - slope * im, moved[rows, 128:] + slope * re))
    return columns_back(out, t)


def columns_spectrum(x, t):
    parts = columns_half(x, t)
    stacked = cat([cat([re, im], 1) for re, im in parts], 0)
    z = right(stacked, t["squares"][WX])
    row = lax.broadcasted_iota(jnp.int32, (8, 128), 0)
    lane = lax.broadcasted_iota(jnp.int32, (8, 128), 1)
    slot = (row == 0) & (lane >= 64) & (lane < 72)
    out = []
    for g in range(len(parts)):
        base = half_rows * g
        z0, z1 = z[base : base + half_rows, :128], z[base : base + half_rows, 128:]
        top0 = jnp.where(slot, roll(z1[:8], 64), z0[:8])
        top1 = jnp.where(row == 0, z0[64:72], z1[:8])
        out.append((cat([top0, z0[8:64]], 0), cat([top1, z1[8:64]], 0)))
    return out


def columns_field(blocks, t):
    row = lax.broadcasted_iota(jnp.int32, (8, 128), 0)
    lane = lax.broadcasted_iota(jnp.int32, (8, 128), 1)
    first = jnp.where(lane < 8, 1.0, jnp.where((lane >= 64) & (lane < 72), 0.0, 2.0))
    stacked = []
    for x0, x1 in blocks:
        top0 = jnp.where(row == 0, first * x0[:8], x0[:8])
        kept = jnp.where(lane < 8, roll(x0[:8], 64), 0.0)
        top1 = jnp.where(row == 0, kept, x1[:8])
        last0 = jnp.where(row == 0, 2.0 * x1[:8], 0.0)
        stacked.append(
            cat(
                [
                    cat([top0, x0[8:], last0], 0),
                    cat([top1, x1[8:], jnp.zeros_like(last0)], 0),
                ],
                1,
            )
        )
    z = right(cat(stacked, 0), t["squares"][WXI])
    parts = []
    for g in range(len(blocks)):
        rows = slice(half_rows * g, half_rows * (g + 1))
        parts.append((z[rows, :128], z[rows, 128:]))
    return columns_back(parts, t)


def waves_forward(x, t):
    blocks = x.shape[0] // 128
    cos, sin = t["twy"][0], t["twy"][1]
    halves = split(x)
    lanes = []
    for table in (WYA, WYB):
        y = product(halves, (t["squares"][table][0], t["squares"][table][1]))
        for b in range(blocks):
            rows = slice(128 * b, 128 * b + 128)
            re, im = turn(y[rows, :128], y[rows, 128:], cos, sin)
            lanes.append(cat([re, im], 0))
    z = left(t["squares"][TY], cat(lanes, 1))
    out = []
    for b in range(blocks):
        for origin in range(2):
            at = 128 * (origin * blocks + b)
            out.append((z[:128, at : at + 128], z[128:, at : at + 128]))
    return out


def waves_back(values, t):
    cos, sin = t["twy"][0], t["twy"][1]
    z = left(t["squares"][TYI], cat([cat([re, im], 0) for re, im in values], 1))
    rows = []
    for v in range(len(values)):
        part = z[:, 128 * v : 128 * v + 128]
        rows.append(cat(turn_back(part[:128], part[128:], cos, sin), 1))
    y = right(cat(rows, 0), t["squares"][WYI])
    return [y[128 * v : 128 * v + 128] for v in range(len(values))]


def roll(x, shift):
    return pltpu.roll(x, shift, 1)


def denominators(me):
    lane = lax.broadcasted_iota(jnp.int32, (128, 128), 1)
    row = lax.broadcasted_iota(jnp.int32, (128, 128), 0)
    k = lane // 16
    first = jnp.where(me == 1, 64, me // 2) + 1024 * jnp.where(me == 1, 0, me % 2)
    a = first + 128 * k
    b = lane % 16 + 16 * row
    packed = (k == 0) & (me == 0)

    def square(index):
        wave = unit * jnp.where(index < n // 2, index, index - n).astype(f32)
        return wave * wave

    out = []
    for index in (a, jnp.where(packed, n // 2, a)):
        ksq = square(index) + square(b)
        out.append(1.0 / (1.0 + step * (ksq * ksq - ksq)))
    return out[0], out[1], packed


ROWS = dict(ug=4, t=2, f=4, wt=4, m=2, n=2, fg=4, q=2, v=2, nx=2)
KEYS = tuple(ROWS)


def kernel(*refs):
    u_ref, t_ref, f_ref = refs[:3]
    tables_hbm = refs[3 : 3 + len(NAMES)]
    refs = refs[3 + len(NAMES) :]
    next_ref, objective_ref, grad_ref, fgrad_ref = refs[:4]
    refs = refs[4:]
    tables = dict(zip(NAMES, refs[: len(NAMES)]))
    refs = refs[len(NAMES) :]
    send = dict(zip(KEYS, refs[: len(KEYS)]))
    refs = refs[len(KEYS) :]
    recv = dict(zip(KEYS, refs[: len(KEYS)]))
    refs = refs[len(KEYS) :]
    part_ref, parts_ref, g1_ref, g2_ref, forced_ref = refs[:5]
    table_sem, send_sem, recv_sem, own_sem = refs[5:]

    me = lax.axis_index("px") * 8 + lax.axis_index("py")
    barrier = pltpu.get_barrier_semaphore()

    def greet(i, carry):
        d = jnp.bitwise_xor(me, i)
        pl.semaphore_signal(barrier, inc=1, device_id=(d // 8, d % 8), device_id_type=MESH)
        return carry

    loads = [
        pltpu.make_async_copy(src, tables[name], table_sem.at[i])
        for i, (name, src) in enumerate(zip(NAMES, tables_hbm))
    ]
    for load in loads:
        load.start()
    lax.fori_loop(1, peers, greet, 0)

    def flat(ref):
        return ref.reshape(ref.shape[0] * ref.shape[1], 128)

    def put(key, row, value):
        flat(send[key])[pl.ds(row, peers, ROWS[key]), :] = value

    def get(key, row, count=peers, stride=None):
        return flat(recv[key])[pl.ds(row, count, stride or ROWS[key]), :]

    def start(key):
        i = KEYS.index(key)
        src, dst = send[key], recv[key]
        pltpu.make_async_copy(src.at[me], dst.at[me], own_sem.at[i]).start()

        def one(j, carry):
            d = jnp.bitwise_xor(me, peers - j)
            pltpu.make_async_remote_copy(
                src.at[d], dst.at[me], send_sem.at[i], recv_sem.at[i],
                device_id=(d // 8, d % 8), device_id_type=MESH,
            ).start()
            return carry

        lax.fori_loop(1, peers, one, 0)

    def whole(key):
        i = KEYS.index(key)
        span = pl.ds(0, peers - 1)
        return pltpu.make_async_remote_copy(
            send[key].at[span], recv[key].at[span], send_sem.at[i], recv_sem.at[i],
            device_id=(0, 0), device_id_type=MESH,
        )

    def arrive(key):
        i = KEYS.index(key)
        pltpu.make_async_copy(send[key].at[me], recv[key].at[me], own_sem.at[i]).wait()
        whole(key).wait_recv()

    def tiles_of(ref):
        return [ref[:, 128 * i : 128 * i + 128] for i in range(16)]

    def put_field(key, row, tiles):
        for g in range(2):
            put(key, row + g, cat(tiles[8 * g : 8 * g + 8], 0).T)

    def get_tiles(key):
        out = []
        for g in range(2):
            block = get(key, g).T
            out += [block[16 * i : 16 * i + 16] for i in range(8)]
        return out

    for load in loads:
        load.wait()
    t = tables
    u_tiles = tiles_of(u_ref)
    put_field("ug", 0, u_tiles)
    put_field("ug", 2, rows_derivative(u_tiles, t))
    put_field("t", 0, tiles_of(t_ref))
    pl.semaphore_wait(barrier, peers - 1)
    start("ug")
    start("t")
    for c in range(2):
        for which in range(2):
            sides = []
            for h in range(2):
                order = range(8) if which == 0 else range(7, -1, -1)
                sides.append(
                    cat([f_ref[c, :, 128 * (8 * h + k) : 128 * (8 * h + k) + 128] for k in order], 0)
                )
            high, low = split(cat(sides, 1))
            dims = (((1,), (1,)), ((), ()))
            place = t["places"][which]
            moved = lax.dot_general(place, high, dims, preferred_element_type=f32)
            moved = moved + lax.dot_general(place, low, dims, preferred_element_type=f32)
            put("f", 2 * which + c, moved)
    start("f")
    r_re, r_im, packed = denominators(me)

    arrive("ug")
    u = cat([get("ug", 0), get("ug", 1)], 1)
    g2 = cat([get("ug", 2), get("ug", 3)], 1)
    g1 = columns_derivative(u, t)
    g1_ref[...] = g1
    g2_ref[...] = g2
    pushed = u + (-0.5 * step) * (g1 * g1 + g2 * g2)
    arrive("t")
    goal = cat([get("t", 0), get("t", 1)], 1)
    for g, blocks in enumerate(columns_spectrum(cat([pushed, goal], 1), t)):
        for h in range(2):
            flat(send["wt"])[pl.ds(4 * h + g, 64, 8), :] = blocks[h]
    start("wt")

    arrive("f")
    own = (get("f", 0), get("f", 1))
    mirror = tuple(jnp.where(me == 0, roll(get("f", 2 + c), 16), get("f", 2 + c)) for c in range(2))
    here, there = waves_back([own, mirror], t)
    lane = lax.broadcasted_iota(jnp.int32, (128, 128), 1)
    column = lane % 64 // 8
    special = (column == 0) & (me == 0)
    for g in range(2):
        a = here[:, 128 * g : 128 * g + 128]
        b = there[:, 128 * g : 128 * g + 128]
        even = 0.5 * jnp.where(lane < 64, a + b, a - b)
        single = jnp.where(lane < 64, a, roll(b, 64))
        forced_ref[:, 128 * g : 128 * g + 128] = step * jnp.where(special, single, even)

    arrive("wt")
    w = cat([get("wt", 0), get("wt", 1)], 1) + forced_ref[...]
    goal = cat([get("wt", 2), get("wt", 3)], 1)
    z_re, z_im, t_re, t_im = waves_forward(cat([w, goal], 0), t)
    next_re = tuple(r_re * z for z in z_re)
    next_im = tuple(r_im * z for z in z_im)
    miss_re = tuple(a - b for a, b in zip(next_re, t_re))
    miss_im = tuple(a - b for a, b in zip(next_im, t_im))
    c_re = tuple((step * r_re) * v for v in miss_re)
    c_im = tuple((step * r_im) * v for v in miss_im)
    join = lambda x, y: (x[0] - y[1], x[1] + y[0])
    part = lambda x, y: (x[0] + y[1], x[1] - y[0])
    coef = join(c_re, c_im)
    m_out, n_out = waves_back([coef, join(next_re, next_im)], t)
    for g in range(2):
        put("m", g, m_out[:, 128 * g : 128 * g + 128])
    start("m")
    for g in range(2):
        put("n", g, n_out[:, 128 * g : 128 * g + 128])
    start("n")
    other = part(c_re, c_im)
    for c in range(2):
        put("fg", c, jnp.where(packed, c_re[c], coef[c]))
        back = jnp.where(packed, c_im[c], other[c])
        put("fg", 2 + c, jnp.where(me == 0, roll(back, 112), back))
    start("fg")
    miss = join(miss_re, miss_im)
    total = jnp.where(packed, 1.0, 2.0) * (miss[0] * miss[0] + miss[1] * miss[1])
    part_ref[...] = jnp.sum(total, axis=0, keepdims=True)
    parts_index = len(KEYS)
    parts_ref[me] = part_ref[...]

    def tell(j, carry):
        d = jnp.bitwise_xor(me, peers - j)
        pltpu.make_async_remote_copy(
            part_ref, parts_ref.at[me], send_sem.at[parts_index], recv_sem.at[parts_index],
            device_id=(d // 8, d % 8), device_id_type=MESH,
        ).start()
        return carry

    lax.fori_loop(1, peers, tell, 0)

    def blocks_of(key):
        return [
            tuple(get(key, 2 * h + g, 64, 4) for h in range(2))
            for g in range(2)
        ]

    arrive("m")
    m = columns_field(blocks_of("m"), t)
    q2 = m * g2_ref[...]
    for g in range(2):
        put("q", g, q2[:, 128 * g : 128 * g + 128])
    start("q")
    v = 4.0 * m + columns_derivative(m * g1_ref[...], t)
    for g in range(2):
        put("v", g, v[:, 128 * g : 128 * g + 128])
    start("v")
    arrive("n")
    stepped = columns_field(blocks_of("n"), t)
    for g in range(2):
        put("nx", g, stepped[:, 128 * g : 128 * g + 128])
    start("nx")

    arrive("fg")
    sides = []
    for which in range(2):
        block = cat([get("fg", 2 * which), get("fg", 2 * which + 1)], 1)
        high, low = split(block)
        place = t["places_t"][which]
        sides.append(dot(place, high) + dot(place, low))
    for h in range(2):
        for c in range(2):
            a = sides[0][128 * h : 128 * h + 128, 128 * c : 128 * c + 128].T
            b = sides[1][128 * h : 128 * h + 128, 128 * c : 128 * c + 128].T
            for k in range(8):
                at = 128 * (8 * h + k)
                fgrad_ref[c, :, at : at + 128] = (
                    a[16 * k : 16 * k + 16] + b[16 * (7 - k) : 16 * (7 - k) + 16]
                )
    pltpu.make_async_remote_copy(
        parts_ref.at[pl.ds(0, peers - 1)], parts_ref.at[pl.ds(0, peers - 1)],
        send_sem.at[parts_index], recv_sem.at[parts_index],
        device_id=(0, 0), device_id_type=MESH,
    ).wait_recv()
    sums = jnp.sum(flat(parts_ref)[...], axis=0, keepdims=True)
    objective_ref[...] = (0.5 / (n * n)) * jnp.sum(sums, axis=1, keepdims=True)
    arrive("q")
    slope = rows_derivative(get_tiles("q"), t)
    arrive("v")
    for i, tile in enumerate(get_tiles("v")):
        grad_ref[:, 128 * i : 128 * i + 128] = tile + slope[i]
    arrive("nx")
    for i, tile in enumerate(get_tiles("nx")):
        next_ref[:, 128 * i : 128 * i + 128] = tile
    for key in KEYS:
        whole(key).wait_send()
    pltpu.make_async_remote_copy(
        parts_ref.at[pl.ds(0, peers - 1)], parts_ref.at[pl.ds(0, peers - 1)],
        send_sem.at[parts_index], recv_sem.at[parts_index],
        device_id=(0, 0), device_id_type=MESH,
    ).wait_send()


def per_device(initial_field, target_field, forcing):
    built = build_tables()
    constants = [jnp.asarray(built[name]) for name in NAMES]
    vmem = pl.BlockSpec(memory_space=pltpu.VMEM)
    anywhere = pl.BlockSpec(memory_space=pl.ANY)
    messages = [pltpu.VMEM((peers, ROWS[key], 128), f32) for key in KEYS]
    next_field, objective, field_grad, forcing_grad = pl.pallas_call(
        kernel,
        out_shape=(
            jax.ShapeDtypeStruct((16, n), f32),
            jax.ShapeDtypeStruct((1, 1), f32),
            jax.ShapeDtypeStruct((16, n), f32),
            jax.ShapeDtypeStruct((2, 16, n), f32),
        ),
        in_specs=[vmem] * 3 + [anywhere] * len(NAMES),
        out_specs=(vmem,) * 4,
        scratch_shapes=[pltpu.VMEM(c.shape, c.dtype) for c in constants]
        + messages
        + messages
        + [
            pltpu.VMEM((1, 128), f32),
            pltpu.VMEM((peers, 1, 128), f32),
            pltpu.VMEM((128, 256), f32),
            pltpu.VMEM((128, 256), f32),
            pltpu.VMEM((128, 256), f32),
            pltpu.SemaphoreType.DMA((len(NAMES),)),
            pltpu.SemaphoreType.DMA((len(KEYS) + 1,)),
            pltpu.SemaphoreType.DMA((len(KEYS) + 1,)),
            pltpu.SemaphoreType.DMA((len(KEYS),)),
        ],
        compiler_params=pltpu.CompilerParams(
            collective_id=0, has_side_effects=True, vmem_limit_bytes=48 * 1024 * 1024
        ),
    )(initial_field[0], target_field[0], forcing, *constants)
    return next_field[None], objective.reshape(()), field_grad[None], forcing_grad


def solution(mesh):
    spec = P(None, ("px", "py"), None)
    return jax.shard_map(
        per_device,
        mesh=mesh,
        in_specs=(spec, spec, spec),
        out_specs=(spec, P(), spec, spec),
        check_vma=False,
    )
```

```python
import math

import jax
import jax.numpy as jnp
import numpy as np
from jax import lax
from jax.experimental import pallas as pl
from jax.experimental.pallas import tpu as pltpu
from jax.sharding import PartitionSpec as P

LOGICAL = pl.DeviceIdType.LOGICAL
f32 = jnp.float32
bf16 = jnp.bfloat16

n = 2048
peers = 128
step = 0.25
unit = 4.0 / n
half_rows = 72


def cplx(table):
    return np.block([[table.real, table.imag], [-table.imag, table.real]])


def signed(count, index):
    return np.where(index < count // 2, index, index - count)


def build_tables():
    s = np.arange(128)
    a1 = np.arange(65)
    theta = 2 * np.pi * np.outer(a1, s) / 128
    td = np.zeros((2 * half_rows, 128))
    td[:65] = np.cos(theta)
    td[half_rows : half_rows + 65] = -np.sin(theta)
    weight = np.where((a1 == 0) | (a1 == 64), 1.0, 2.0) / 128
    ti = np.zeros((128, 2 * half_rows))
    ti[:, :65] = (np.cos(theta) * weight[:, None]).T
    ti[:, half_rows : half_rows + 65] = (-np.sin(theta) * weight[:, None]).T

    def derivative(length, factor):
        freq = signed(length, s[:length]).astype(float) * factor
        inner = np.where(s[:length] == length // 2, 0.0, freq)
        gap = np.subtract.outer(s[:length], s[:length])
        waves = np.exp(2j * np.pi * gap[:, :, None] * s[:length] / length)
        smooth = (waves * (1j * inner)).sum(-1).real / length
        nyquist = freq[length // 2] * (-1.0) ** gap / length
        return (smooth + 1j * nyquist).T

    root = 1.0 / math.sqrt(n)
    mx = cplx(np.kron(np.eye(8), derivative(16, unit * 128)))
    my = cplx(derivative(128, unit * 16) / 16)

    w16 = np.exp(-2j * np.pi * np.outer(s[:16], s[:16]) / 16)
    eye8 = np.eye(8)
    forward = w16.reshape(16, 2, 8)
    parts = np.zeros((2, 8, 16, 2, 2, 8, 8))
    for y in range(8):
        parts[0, y, :, :, 0, :, y] = forward.real
        parts[0, y, :, :, 1, :, y] = forward.imag
        parts[1, y, :, :, 0, :, y] = -forward.imag
        parts[1, y, :, :, 1, :, y] = forward.real
    wx = parts.reshape(256, 256) * root
    back = w16.conj().T.reshape(2, 8, 16)
    parts = np.zeros((2, 2, 8, 8, 2, 8, 16))
    for y in range(8):
        parts[:, 0, :, y, 0, y, :] = back.real
        parts[:, 0, :, y, 1, y, :] = back.imag
        parts[:, 1, :, y, 0, y, :] = -back.imag
        parts[:, 1, :, y, 1, y, :] = back.real
    wxi = parts.reshape(256, 256) * (128 * root)
    forward = w16.reshape(2, 8, 16)
    parts = np.zeros((2, 2, 8, 8, 2, 2, 8, 16))
    for k in range(8):
        for c in range(2):
            parts[:, c, k, :, c, 0, k, :] = forward.real
            parts[:, c, k, :, c, 1, k, :] = forward.imag
    wy = parts.reshape(256, 512)
    back = w16.conj().T.reshape(16, 2, 8)
    parts = np.zeros((2, 8, 16, 2, 2, 8, 8))
    for k in range(8):
        parts[0, k, :, :, 0, k, :] = back.real
        parts[0, k, :, :, 1, k, :] = back.imag
        parts[1, k, :, :, 0, k, :] = -back.imag
        parts[1, k, :, :, 1, k, :] = back.real
    wyi = parts.reshape(256, 256)
    f128 = np.exp(-2j * np.pi * np.outer(s, s) / 128) * root
    ty = cplx(f128).T
    tyi = cplx(f128.conj()).T
    squares = np.stack([mx, my, wx, wxi, wy[:, :256], wy[:, 256:], wyi, ty, tyi])

    own = np.zeros((128, 2, 128))
    mirror = np.zeros((128, 2, 128))
    for e in range(128):
        h, a = e % 2, e // 2
        if e == 0:
            own[e, 0, 0] = mirror[e, 1, 0] = 1
        elif e == 1:
            own[e, 0, 64] = mirror[e, 1, 64] = 1
        else:
            own[e, h, a] = mirror[e, 1 - h, 128 - a] = 1
    places = np.stack([own.reshape(128, 256), mirror.reshape(128, 256)])

    row = np.arange(half_rows)[:, None]
    lane = np.arange(128)[None, :]
    twx = 2 * np.pi * row * (lane % 16) / n
    twy = 2 * np.pi * np.arange(128)[:, None] * (lane % 16) / n
    twr = 2 * np.pi * np.arange(16)[:, None] * lane / n
    both = lambda t: np.stack([np.cos(t), np.sin(t)]).astype(np.float32)

    def halves(t):
        high = t.astype(np.float32).astype(bf16)
        low = (t - high.astype(np.float64)).astype(np.float32).astype(bf16)
        return high, low

    return dict(
        squares=np.stack(halves(squares), axis=1),
        td=np.stack(halves(td)),
        ti=np.stack(halves(ti)),
        places=places.astype(np.float32).astype(bf16),
        places_t=places.transpose(0, 2, 1).astype(np.float32).astype(bf16),
        twx=both(twx),
        twy=both(twy),
        twr=both(twr),
    )


MX, MY, WX, WXI, WYA, WYB, WYI, TY, TYI = range(9)
NAMES = ("squares", "td", "ti", "places", "places_t", "twx", "twy", "twr")


def split(x):
    high = x.astype(bf16)
    return high, (x - high.astype(f32)).astype(bf16)


def dot(a, b):
    return jnp.dot(a, b, preferred_element_type=f32)


def product(a, b):
    return dot(a[0], b[0]) + (dot(a[0], b[1]) + dot(a[1], b[0]))


def left(table, x):
    return product((table[0], table[1]), split(x))


def right(x, table):
    return product(split(x), (table[0], table[1]))


def cat(parts, axis):
    return jnp.concatenate(parts, axis=axis)


def turn(re, im, cos, sin):
    return re * cos + im * sin, im * cos - re * sin


def turn_back(re, im, cos, sin):
    return re * cos - im * sin, im * cos + re * sin


def real_dft(values):
    count = len(values)
    if count == 2:
        return [(values[0] + values[1], None), (values[0] - values[1], None)]
    even, odd = real_dft(values[0::2]), real_dft(values[1::2])
    quarter = count // 4
    out = [None] * (count // 2 + 1)
    for k in range(quarter + 1):
        (er, ei), (tr, ti) = even[k], odd[k]
        if k == quarter:
            out[k] = (er, -tr)
            continue
        if k > 0:
            c, s = math.cos(2 * math.pi * k / count), math.sin(2 * math.pi * k / count)
            tr, ti = (tr * c + ti * s, ti * c - tr * s) if ti is not None else (tr * c, tr * -s)
        if k == 0:
            out[0], out[count // 2] = (er + tr, None), (er - tr, None)
        else:
            ei = 0.0 if ei is None else ei
            out[k] = (er + tr, ei + ti)
            out[count // 2 - k] = (er - tr, ti - ei)
    return out


def real_idft(spectrum):
    count = 2 * (len(spectrum) - 1)
    if count == 2:
        return [spectrum[0][0] + spectrum[1][0], spectrum[0][0] - spectrum[1][0]]
    quarter = count // 4
    even, odd = [], []
    for k in range(quarter + 1):
        re, im = spectrum[k]
        if k == 0:
            other = spectrum[count // 2][0]
            even.append((re + other, None))
            odd.append((re - other, None))
        elif k == quarter:
            even.append((2.0 * re, None))
            odd.append((-2.0 * im, None))
        else:
            hr, hi = spectrum[count // 2 - k]
            even.append((re + hr, im - hi))
            dr, di = re - hr, im + hi
            c, s = math.cos(2 * math.pi * k / count), math.sin(2 * math.pi * k / count)
            odd.append((dr * c - di * s, dr * s + di * c))
    xs, ys = real_idft(even), real_idft(odd)
    return [v for pair in zip(xs, ys) for v in pair]


def rows_derivative(tiles, t):
    cos, sin = t["twr"][0], t["twr"][1]
    turned = []
    for k, (re, im) in enumerate(real_dft(tiles)):
        c, s = cos[k : k + 1], sin[k : k + 1]
        if k == 0:
            turned.append((re, jnp.zeros_like(re)))
        elif im is None:
            turned.append((re * c, -re * s))
        else:
            turned.append(turn(re, im, c, s))
    re_rows = cat([v[0] for v in turned], 0)
    im_rows = cat([v[1] for v in turned], 0)
    moved = right(cat([re_rows, im_rows], 1), t["squares"][MY])
    out = []
    for k, (re, im) in enumerate(turned):
        mr = moved[16 * k : 16 * k + 16, :128] - (unit / 16 * k) * im
        mi = moved[16 * k : 16 * k + 16, 128:] + (unit / 16 * k) * re
        out.append(turn_back(mr, mi, cos[k : k + 1], sin[k : k + 1]))
    return real_idft(out)


def columns_half(x, t):
    y = left(t["td"], x)
    cos, sin = t["twx"][0], t["twx"][1]
    out = []
    for g in range(x.shape[1] // 128):
        part = y[:, 128 * g : 128 * g + 128]
        out.append(turn(part[:half_rows], part[half_rows:], cos, sin))
    return out


def columns_back(parts, t):
    cos, sin = t["twx"][0], t["twx"][1]
    cols = []
    for re, im in parts:
        br, bi = turn_back(re, im, cos, sin)
        cols.append(cat([br, bi], 0))
    return left(t["ti"], cat(cols, 1))


def columns_derivative(x, t):
    parts = columns_half(x, t)
    stacked = cat([cat([re, im], 1) for re, im in parts], 0)
    moved = right(stacked, t["squares"][MX])
    slope = unit * lax.broadcasted_iota(jnp.int32, (half_rows, 128), 0).astype(f32)
    out = []
    for g, (re, im) in enumerate(parts):
        rows = slice(half_rows * g, half_rows * (g + 1))
        out.append((moved[rows, :128] - slope * im, moved[rows, 128:] + slope * re))
    return columns_back(out, t)


def columns_spectrum(x, t):
    parts = columns_half(x, t)
    stacked = cat([cat([re, im], 1) for re, im in parts], 0)
    z = right(stacked, t["squares"][WX])
    row = lax.broadcasted_iota(jnp.int32, (8, 128), 0)
    lane = lax.broadcasted_iota(jnp.int32, (8, 128), 1)
    slot = (row == 0) & (lane >= 64) & (lane < 72)
    out = []
    for g in range(len(parts)):
        base = half_rows * g
        z0, z1 = z[base : base + half_rows, :128], z[base : base + half_rows, 128:]
        top0 = jnp.where(slot, roll(z1[:8], 64), z0[:8])
        top1 = jnp.where(row == 0, z0[64:72], z1[:8])
        out.append((cat([top0, z0[8:64]], 0), cat([top1, z1[8:64]], 0)))
    return out


def columns_field(blocks, t):
    row = lax.broadcasted_iota(jnp.int32, (8, 128), 0)
    lane = lax.broadcasted_iota(jnp.int32, (8, 128), 1)
    first = jnp.where(lane < 8, 1.0, jnp.where((lane >= 64) & (lane < 72), 0.0, 2.0))
    stacked = []
    for x0, x1 in blocks:
        top0 = jnp.where(row == 0, first * x0[:8], x0[:8])
        kept = jnp.where(lane < 8, roll(x0[:8], 64), 0.0)
        top1 = jnp.where(row == 0, kept, x1[:8])
        last0 = jnp.where(row == 0, 2.0 * x1[:8], 0.0)
        stacked.append(
            cat(
                [
                    cat([top0, x0[8:], last0], 0),
                    cat([top1, x1[8:], jnp.zeros_like(last0)], 0),
                ],
                1,
            )
        )
    z = right(cat(stacked, 0), t["squares"][WXI])
    parts = []
    for g in range(len(blocks)):
        rows = slice(half_rows * g, half_rows * (g + 1))
        parts.append((z[rows, :128], z[rows, 128:]))
    return columns_back(parts, t)


def waves_forward(x, t):
    blocks = x.shape[0] // 128
    cos, sin = t["twy"][0], t["twy"][1]
    halves = split(x)
    lanes = []
    for table in (WYA, WYB):
        y = product(halves, (t["squares"][table][0], t["squares"][table][1]))
        for b in range(blocks):
            rows = slice(128 * b, 128 * b + 128)
            re, im = turn(y[rows, :128], y[rows, 128:], cos, sin)
            lanes.append(cat([re, im], 0))
    z = left(t["squares"][TY], cat(lanes, 1))
    out = []
    for b in range(blocks):
        for origin in range(2):
            at = 128 * (origin * blocks + b)
            out.append((z[:128, at : at + 128], z[128:, at : at + 128]))
    return out


def waves_back(values, t):
    cos, sin = t["twy"][0], t["twy"][1]
    z = left(t["squares"][TYI], cat([cat([re, im], 0) for re, im in values], 1))
    rows = []
    for v in range(len(values)):
        part = z[:, 128 * v : 128 * v + 128]
        rows.append(cat(turn_back(part[:128], part[128:], cos, sin), 1))
    y = right(cat(rows, 0), t["squares"][WYI])
    return [y[128 * v : 128 * v + 128] for v in range(len(values))]


def roll(x, shift):
    return pltpu.roll(x, shift, 1)


def denominators(me):
    lane = lax.broadcasted_iota(jnp.int32, (128, 128), 1)
    row = lax.broadcasted_iota(jnp.int32, (128, 128), 0)
    k = lane // 16
    first = jnp.where(me == 1, 64, me // 2) + 1024 * jnp.where(me == 1, 0, me % 2)
    a = first + 128 * k
    b = lane % 16 + 16 * row
    packed = (k == 0) & (me == 0)

    def square(index):
        wave = unit * jnp.where(index < n // 2, index, index - n).astype(f32)
        return wave * wave

    out = []
    for index in (a, jnp.where(packed, n // 2, a)):
        ksq = square(index) + square(b)
        out.append(1.0 / (1.0 + step * (ksq * ksq - ksq)))
    return out[0], out[1], packed


ROWS = dict(ug=4, t=2, f=4, wt=4, m=2, n=2, fg=4, q=2, v=2, nx=2)
KEYS = tuple(ROWS)


RECEIVED = tuple(key for key in KEYS if key not in ("v", "nx"))


def kernel(*refs):
    fields_hbm = refs[:3]
    tables_hbm = refs[3 : 3 + len(NAMES)]
    refs = refs[3 + len(NAMES) :]
    objective_ref, slope_ref, fgrad_ref = refs[:3]
    recv = dict(zip(("v", "nx"), refs[3:5]))
    refs = refs[5:]
    u_ref, t_ref, f_ref = refs[:3]
    refs = refs[3:]
    tables = dict(zip(NAMES, refs[: len(NAMES)]))
    refs = refs[len(NAMES) :]
    send = dict(zip(KEYS, refs[: len(KEYS)]))
    refs = refs[len(KEYS) :]
    recv.update(zip(RECEIVED, refs[: len(RECEIVED)]))
    refs = refs[len(RECEIVED) :]
    part_ref, parts_ref, g1_ref, g2_ref, forced_ref = refs[:5]
    table_sem, send_sem, recv_sem, own_sem = refs[5:]

    me = lax.axis_index("px") * 8 + lax.axis_index("py")
    barrier = pltpu.get_barrier_semaphore()

    def greet(i, carry):
        d = jnp.bitwise_xor(me, peers - i)
        pl.semaphore_signal(barrier, inc=1, device_id=d, device_id_type=LOGICAL)
        return carry

    lax.fori_loop(1, peers, greet, 0, unroll=4)
    loads = [
        pltpu.make_async_copy(src, dst, table_sem.at[i])
        for i, (src, dst) in enumerate(
            zip(fields_hbm + tables_hbm, [u_ref, t_ref, f_ref] + [tables[k] for k in NAMES])
        )
    ]
    for load in loads:
        load.start()

    def flat(ref):
        return ref.reshape(ref.shape[0] * ref.shape[1], 128)

    def put(key, row, value):
        flat(send[key])[pl.ds(row, peers, ROWS[key]), :] = value

    def get(key, row, count=peers, stride=None):
        return flat(recv[key])[pl.ds(row, count, stride or ROWS[key]), :]

    def start(key):
        i = KEYS.index(key)
        src, dst = send[key], recv[key]
        pltpu.make_async_copy(src.at[me], dst.at[me], own_sem.at[i]).start()

        def one(j, carry):
            d = jnp.bitwise_xor(me, peers - j)
            pltpu.make_async_remote_copy(
                src.at[d], dst.at[me], send_sem.at[i], recv_sem.at[i],
                device_id=d, device_id_type=LOGICAL,
            ).start()
            return carry

        lax.fori_loop(1, peers, one, 0, unroll=4)

    def whole(key):
        i = KEYS.index(key)
        span = pl.ds(0, peers - 1)
        return pltpu.make_async_remote_copy(
            send[key].at[span], recv[key].at[span], send_sem.at[i], recv_sem.at[i],
            device_id=0, device_id_type=LOGICAL,
        )

    def arrive(key):
        i = KEYS.index(key)
        pltpu.make_async_copy(send[key].at[me], recv[key].at[me], own_sem.at[i]).wait()
        whole(key).wait_recv()

    def tiles_of(ref):
        return [ref[:, 128 * i : 128 * i + 128] for i in range(16)]

    def put_field(key, row, tiles):
        for g in range(2):
            put(key, row + g, cat(tiles[8 * g : 8 * g + 8], 0).T)

    def get_tiles(key):
        out = []
        for g in range(2):
            block = get(key, g).T
            out += [block[16 * i : 16 * i + 16] for i in range(8)]
        return out

    for load in loads:
        load.wait()
    t = tables
    u_tiles = tiles_of(u_ref)
    put_field("ug", 0, u_tiles)
    put_field("ug", 2, rows_derivative(u_tiles, t))
    put_field("t", 0, tiles_of(t_ref))
    pl.semaphore_wait(barrier, peers - 1)
    start("ug")
    start("t")
    for c in range(2):
        for which in range(2):
            sides = []
            for h in range(2):
                order = range(8) if which == 0 else range(7, -1, -1)
                sides.append(
                    cat([f_ref[c, :, 128 * (8 * h + k) : 128 * (8 * h + k) + 128] for k in order], 0)
                )
            high, low = split(cat(sides, 1))
            dims = (((1,), (1,)), ((), ()))
            place = t["places"][which]
            moved = lax.dot_general(place, high, dims, preferred_element_type=f32)
            moved = moved + lax.dot_general(place, low, dims, preferred_element_type=f32)
            put("f", 2 * which + c, moved)
    start("f")
    r_re, r_im, packed = denominators(me)

    arrive("ug")
    u = cat([get("ug", 0), get("ug", 1)], 1)
    g2 = cat([get("ug", 2), get("ug", 3)], 1)
    g1 = columns_derivative(u, t)
    g1_ref[...] = g1
    g2_ref[...] = g2
    pushed = u + (-0.5 * step) * (g1 * g1 + g2 * g2)
    arrive("t")
    goal = cat([get("t", 0), get("t", 1)], 1)
    for g, blocks in enumerate(columns_spectrum(cat([pushed, goal], 1), t)):
        for h in range(2):
            flat(send["wt"])[pl.ds(4 * h + g, 64, 8), :] = blocks[h]
    start("wt")

    arrive("f")
    own = (get("f", 0), get("f", 1))
    mirror = tuple(jnp.where(me == 0, roll(get("f", 2 + c), 16), get("f", 2 + c)) for c in range(2))
    here, there = waves_back([own, mirror], t)
    lane = lax.broadcasted_iota(jnp.int32, (128, 128), 1)
    column = lane % 64 // 8
    special = (column == 0) & (me == 0)
    for g in range(2):
        a = here[:, 128 * g : 128 * g + 128]
        b = there[:, 128 * g : 128 * g + 128]
        even = 0.5 * jnp.where(lane < 64, a + b, a - b)
        single = jnp.where(lane < 64, a, roll(b, 64))
        forced_ref[:, 128 * g : 128 * g + 128] = step * jnp.where(special, single, even)

    arrive("wt")
    w = cat([get("wt", 0), get("wt", 1)], 1) + forced_ref[...]
    goal = cat([get("wt", 2), get("wt", 3)], 1)
    z_re, z_im, t_re, t_im = waves_forward(cat([w, goal], 0), t)
    next_re = tuple(r_re * z for z in z_re)
    next_im = tuple(r_im * z for z in z_im)
    miss_re = tuple(a - b for a, b in zip(next_re, t_re))
    miss_im = tuple(a - b for a, b in zip(next_im, t_im))
    c_re = tuple((step * r_re) * v for v in miss_re)
    c_im = tuple((step * r_im) * v for v in miss_im)
    join = lambda x, y: (x[0] - y[1], x[1] + y[0])
    part = lambda x, y: (x[0] + y[1], x[1] - y[0])
    coef = join(c_re, c_im)
    m_out, n_out = waves_back([coef, join(next_re, next_im)], t)
    for g in range(2):
        put("m", g, m_out[:, 128 * g : 128 * g + 128])
    start("m")
    for g in range(2):
        put("n", g, n_out[:, 128 * g : 128 * g + 128])
    start("n")
    other = part(c_re, c_im)
    for c in range(2):
        put("fg", c, jnp.where(packed, c_re[c], coef[c]))
        back = jnp.where(packed, c_im[c], other[c])
        put("fg", 2 + c, jnp.where(me == 0, roll(back, 112), back))
    start("fg")
    miss = join(miss_re, miss_im)
    total = jnp.where(packed, 1.0, 2.0) * (miss[0] * miss[0] + miss[1] * miss[1])
    part_ref[...] = jnp.sum(total, axis=0, keepdims=True)
    parts_index = len(KEYS)
    parts_ref[me] = part_ref[...]

    def tell(j, carry):
        d = jnp.bitwise_xor(me, peers - j)
        pltpu.make_async_remote_copy(
            part_ref, parts_ref.at[me], send_sem.at[parts_index], recv_sem.at[parts_index],
            device_id=d, device_id_type=LOGICAL,
        ).start()
        return carry

    lax.fori_loop(1, peers, tell, 0, unroll=4)

    def blocks_of(key):
        return [
            tuple(get(key, 2 * h + g, 64, 4) for h in range(2))
            for g in range(2)
        ]

    arrive("m")
    m = columns_field(blocks_of("m"), t)
    q2 = m * g2_ref[...]
    for g in range(2):
        put("q", g, q2[:, 128 * g : 128 * g + 128])
    start("q")
    v = 4.0 * m + columns_derivative(m * g1_ref[...], t)
    for g in range(2):
        put("v", g, v[:, 128 * g : 128 * g + 128])
    start("v")
    arrive("n")
    stepped = columns_field(blocks_of("n"), t)
    for g in range(2):
        put("nx", g, stepped[:, 128 * g : 128 * g + 128])
    start("nx")

    arrive("fg")
    sides = []
    for which in range(2):
        block = cat([get("fg", 2 * which), get("fg", 2 * which + 1)], 1)
        high, low = split(block)
        place = t["places_t"][which]
        sides.append(dot(place, high) + dot(place, low))
    for h in range(2):
        for c in range(2):
            a = sides[0][128 * h : 128 * h + 128, 128 * c : 128 * c + 128].T
            b = sides[1][128 * h : 128 * h + 128, 128 * c : 128 * c + 128].T
            for k in range(8):
                at = 128 * (8 * h + k)
                fgrad_ref[c, :, at : at + 128] = (
                    a[16 * k : 16 * k + 16] + b[16 * (7 - k) : 16 * (7 - k) + 16]
                )
    pltpu.make_async_remote_copy(
        parts_ref.at[pl.ds(0, peers - 1)], parts_ref.at[pl.ds(0, peers - 1)],
        send_sem.at[parts_index], recv_sem.at[parts_index],
        device_id=0, device_id_type=LOGICAL,
    ).wait_recv()
    sums = jnp.sum(flat(parts_ref)[...], axis=0, keepdims=True)
    objective_ref[...] = (0.5 / (n * n)) * jnp.sum(sums, axis=1, keepdims=True)
    arrive("q")
    for i, tile in enumerate(rows_derivative(get_tiles("q"), t)):
        slope_ref[:, 128 * i : 128 * i + 128] = tile
    arrive("v")
    arrive("nx")
    for key in KEYS:
        whole(key).wait_send()
    pltpu.make_async_remote_copy(
        parts_ref.at[pl.ds(0, peers - 1)], parts_ref.at[pl.ds(0, peers - 1)],
        send_sem.at[parts_index], recv_sem.at[parts_index],
        device_id=0, device_id_type=LOGICAL,
    ).wait_send()


def finish(
    total_ref, slope_ref, fgrad_ref, v_ref, nx_ref,
    objective_out, grad_out, next_out, fgrad_out, grad, nexts, sems,
):
    objective_out[...] = total_ref[...]
    copies = [
        pltpu.make_async_copy(src, dst, sems.at[i])
        for i, (src, dst) in enumerate(
            ((fgrad_ref, fgrad_out), (grad, grad_out), (nexts, next_out))
        )
    ]
    copies[0].start()
    for ref, out, i in ((v_ref, grad, 1), (nx_ref, nexts, 2)):
        for g in range(2):
            block = ref.reshape(2 * peers, 128)[pl.ds(g, peers, 2), :].T
            for k in range(8):
                at = 128 * (8 * g + k)
                tile = block[16 * k : 16 * k + 16]
                if i == 1:
                    tile = tile + slope_ref[:, at : at + 128]
                out[:, at : at + 128] = tile
        copies[i].start()
    for copy in copies:
        copy.wait()


def per_device(initial_field, target_field, forcing):
    built = build_tables()
    constants = [jnp.asarray(built[name]) for name in NAMES]
    vmem = pl.BlockSpec(memory_space=pltpu.VMEM)
    hbm = pl.BlockSpec(memory_space=pltpu.HBM)
    message = lambda key: pltpu.VMEM((peers, ROWS[key], 128), f32)
    operands = tuple(
        pltpu.with_memory_space_constraint(x, pltpu.HBM)
        for x in (initial_field[0], target_field[0], forcing, *constants)
    )
    field = jax.ShapeDtypeStruct((16, n), f32)
    both = jax.ShapeDtypeStruct((2, 16, n), f32)
    landing = jax.ShapeDtypeStruct((peers, 2, 128), f32)
    total, slope, forcing_rows, v, nx = pl.pallas_call(
        kernel,
        out_shape=(jax.ShapeDtypeStruct((1, 1), f32), field, both, landing, landing),
        in_specs=[hbm] * len(operands),
        out_specs=(vmem,) * 5,
        scratch_shapes=[pltpu.VMEM(x.shape, x.dtype) for x in operands]
        + [message(key) for key in KEYS]
        + [message(key) for key in RECEIVED]
        + [
            pltpu.VMEM((1, 128), f32),
            pltpu.VMEM((peers, 1, 128), f32),
            pltpu.VMEM((128, 256), f32),
            pltpu.VMEM((128, 256), f32),
            pltpu.VMEM((128, 256), f32),
            pltpu.SemaphoreType.DMA((len(operands),)),
            pltpu.SemaphoreType.DMA((len(KEYS) + 1,)),
            pltpu.SemaphoreType.DMA((len(KEYS) + 1,)),
            pltpu.SemaphoreType.DMA((len(KEYS),)),
        ],
        compiler_params=pltpu.CompilerParams(
            collective_id=0, has_side_effects=True, vmem_limit_bytes=32 * 1024 * 1024
        ),
    )(*operands)
    objective, field_grad, next_field, forcing_grad = pl.pallas_call(
        finish,
        out_shape=(jax.ShapeDtypeStruct((1, 1), f32), field, field, both),
        in_specs=[vmem] * 5,
        out_specs=(vmem,) + (hbm,) * 3,
        scratch_shapes=[
            pltpu.VMEM((16, n), f32),
            pltpu.VMEM((16, n), f32),
            pltpu.SemaphoreType.DMA((3,)),
        ],
        compiler_params=pltpu.CompilerParams(vmem_limit_bytes=8 * 1024 * 1024),
    )(total, slope, forcing_rows, v, nx)
    return next_field[None], objective.reshape(()), field_grad[None], forcing_grad


def solution(mesh):
    spec = P(None, ("px", "py"), None)
    return jax.shard_map(
        per_device,
        mesh=mesh,
        in_specs=(spec, spec, spec),
        out_specs=(spec, P(), spec, spec),
        check_vma=False,
    )
```

```python
import math

import jax
import jax.numpy as jnp
import numpy as np
from jax import lax
from jax.experimental import pallas as pl
from jax.experimental.pallas import tpu as pltpu
from jax.sharding import PartitionSpec as P

LOGICAL = pl.DeviceIdType.LOGICAL
f32 = jnp.float32
bf16 = jnp.bfloat16

n = 2048
peers = 128
step = 0.25
unit = 4.0 / n
half_rows = 72


def cplx(table):
    return np.block([[table.real, table.imag], [-table.imag, table.real]])


def signed(count, index):
    return np.where(index < count // 2, index, index - count)


def build_tables():
    s = np.arange(128)
    a1 = np.arange(65)
    theta = 2 * np.pi * np.outer(a1, s) / 128
    td = np.zeros((2 * half_rows, 128))
    td[:65] = np.cos(theta)
    td[half_rows : half_rows + 65] = -np.sin(theta)
    weight = np.where((a1 == 0) | (a1 == 64), 1.0, 2.0) / 128
    ti = np.zeros((128, 2 * half_rows))
    ti[:, :65] = (np.cos(theta) * weight[:, None]).T
    ti[:, half_rows : half_rows + 65] = (-np.sin(theta) * weight[:, None]).T

    def derivative(length, factor):
        freq = signed(length, s[:length]).astype(float) * factor
        inner = np.where(s[:length] == length // 2, 0.0, freq)
        gap = np.subtract.outer(s[:length], s[:length])
        waves = np.exp(2j * np.pi * gap[:, :, None] * s[:length] / length)
        smooth = (waves * (1j * inner)).sum(-1).real / length
        nyquist = freq[length // 2] * (-1.0) ** gap / length
        return (smooth + 1j * nyquist).T

    root = 1.0 / math.sqrt(n)
    mx = cplx(np.kron(np.eye(8), derivative(16, unit * 128)))
    my = cplx(derivative(128, unit * 16) / 16)

    w16 = np.exp(-2j * np.pi * np.outer(s[:16], s[:16]) / 16)
    eye8 = np.eye(8)
    forward = w16.reshape(16, 2, 8)
    parts = np.zeros((2, 8, 16, 2, 2, 8, 8))
    for y in range(8):
        parts[0, y, :, :, 0, :, y] = forward.real
        parts[0, y, :, :, 1, :, y] = forward.imag
        parts[1, y, :, :, 0, :, y] = -forward.imag
        parts[1, y, :, :, 1, :, y] = forward.real
    wx = parts.reshape(256, 256) * root
    back = w16.conj().T.reshape(2, 8, 16)
    parts = np.zeros((2, 2, 8, 8, 2, 8, 16))
    for y in range(8):
        parts[:, 0, :, y, 0, y, :] = back.real
        parts[:, 0, :, y, 1, y, :] = back.imag
        parts[:, 1, :, y, 0, y, :] = -back.imag
        parts[:, 1, :, y, 1, y, :] = back.real
    wxi = parts.reshape(256, 256) * (128 * root)
    forward = w16.reshape(2, 8, 16)
    parts = np.zeros((2, 2, 8, 8, 2, 2, 8, 16))
    for k in range(8):
        for c in range(2):
            parts[:, c, k, :, c, 0, k, :] = forward.real
            parts[:, c, k, :, c, 1, k, :] = forward.imag
    wy = parts.reshape(256, 512)
    back = w16.conj().T.reshape(16, 2, 8)
    parts = np.zeros((2, 8, 16, 2, 2, 8, 8))
    for k in range(8):
        parts[0, k, :, :, 0, k, :] = back.real
        parts[0, k, :, :, 1, k, :] = back.imag
        parts[1, k, :, :, 0, k, :] = -back.imag
        parts[1, k, :, :, 1, k, :] = back.real
    wyi = parts.reshape(256, 256)
    f128 = np.exp(-2j * np.pi * np.outer(s, s) / 128) * root
    ty = cplx(f128).T
    tyi = cplx(f128.conj()).T
    squares = np.stack([mx, my, wx, wxi, wy[:, :256], wy[:, 256:], wyi, ty, tyi])

    own = np.zeros((128, 2, 128))
    mirror = np.zeros((128, 2, 128))
    for e in range(128):
        h, a = e % 2, e // 2
        if e == 0:
            own[e, 0, 0] = mirror[e, 1, 0] = 1
        elif e == 1:
            own[e, 0, 64] = mirror[e, 1, 64] = 1
        else:
            own[e, h, a] = mirror[e, 1 - h, 128 - a] = 1
    places = np.stack([own.reshape(128, 256), mirror.reshape(128, 256)])

    row = np.arange(half_rows)[:, None]
    lane = np.arange(128)[None, :]
    twx = 2 * np.pi * row * (lane % 16) / n
    twy = 2 * np.pi * np.arange(128)[:, None] * (lane % 16) / n
    twr = 2 * np.pi * np.arange(16)[:, None] * lane / n
    both = lambda t: np.stack([np.cos(t), np.sin(t)]).astype(np.float32)

    def halves(t):
        high = t.astype(np.float32).astype(bf16)
        low = (t - high.astype(np.float64)).astype(np.float32).astype(bf16)
        return high, low

    return dict(
        squares=np.stack(halves(squares), axis=1),
        td=np.stack(halves(td)),
        ti=np.stack(halves(ti)),
        places=places.astype(np.float32).astype(bf16),
        places_t=places.transpose(0, 2, 1).astype(np.float32).astype(bf16),
        twx=both(twx),
        twy=both(twy),
        twr=both(twr),
    )


MX, MY, WX, WXI, WYA, WYB, WYI, TY, TYI = range(9)
NAMES = ("squares", "td", "ti", "places", "places_t", "twx", "twy", "twr")


def split(x):
    high = x.astype(bf16)
    return high, (x - high.astype(f32)).astype(bf16)


def dot(a, b):
    return jnp.dot(a, b, preferred_element_type=f32)


def product(a, b):
    return dot(a[0], b[0]) + (dot(a[0], b[1]) + dot(a[1], b[0]))


def left(table, x):
    return product((table[0], table[1]), split(x))


def right(x, table):
    return product(split(x), (table[0], table[1]))


def cat(parts, axis):
    return jnp.concatenate(parts, axis=axis)


def turn(re, im, cos, sin):
    return re * cos + im * sin, im * cos - re * sin


def turn_back(re, im, cos, sin):
    return re * cos - im * sin, im * cos + re * sin


def real_dft(values):
    count = len(values)
    if count == 2:
        return [(values[0] + values[1], None), (values[0] - values[1], None)]
    even, odd = real_dft(values[0::2]), real_dft(values[1::2])
    quarter = count // 4
    out = [None] * (count // 2 + 1)
    for k in range(quarter + 1):
        (er, ei), (tr, ti) = even[k], odd[k]
        if k == quarter:
            out[k] = (er, -tr)
            continue
        if k > 0:
            c, s = math.cos(2 * math.pi * k / count), math.sin(2 * math.pi * k / count)
            tr, ti = (tr * c + ti * s, ti * c - tr * s) if ti is not None else (tr * c, tr * -s)
        if k == 0:
            out[0], out[count // 2] = (er + tr, None), (er - tr, None)
        else:
            ei = 0.0 if ei is None else ei
            out[k] = (er + tr, ei + ti)
            out[count // 2 - k] = (er - tr, ti - ei)
    return out


def real_idft(spectrum):
    count = 2 * (len(spectrum) - 1)
    if count == 2:
        return [spectrum[0][0] + spectrum[1][0], spectrum[0][0] - spectrum[1][0]]
    quarter = count // 4
    even, odd = [], []
    for k in range(quarter + 1):
        re, im = spectrum[k]
        if k == 0:
            other = spectrum[count // 2][0]
            even.append((re + other, None))
            odd.append((re - other, None))
        elif k == quarter:
            even.append((2.0 * re, None))
            odd.append((-2.0 * im, None))
        else:
            hr, hi = spectrum[count // 2 - k]
            even.append((re + hr, im - hi))
            dr, di = re - hr, im + hi
            c, s = math.cos(2 * math.pi * k / count), math.sin(2 * math.pi * k / count)
            odd.append((dr * c - di * s, dr * s + di * c))
    xs, ys = real_idft(even), real_idft(odd)
    return [v for pair in zip(xs, ys) for v in pair]


def rows_derivative(tiles, t):
    cos, sin = t["twr"][0], t["twr"][1]
    turned = []
    for k, (re, im) in enumerate(real_dft(tiles)):
        c, s = cos[k : k + 1], sin[k : k + 1]
        if k == 0:
            turned.append((re, jnp.zeros_like(re)))
        elif im is None:
            turned.append((re * c, -re * s))
        else:
            turned.append(turn(re, im, c, s))
    re_rows = cat([v[0] for v in turned], 0)
    im_rows = cat([v[1] for v in turned], 0)
    moved = right(cat([re_rows, im_rows], 1), t["squares"][MY])
    out = []
    for k, (re, im) in enumerate(turned):
        mr = moved[16 * k : 16 * k + 16, :128] - (unit / 16 * k) * im
        mi = moved[16 * k : 16 * k + 16, 128:] + (unit / 16 * k) * re
        out.append(turn_back(mr, mi, cos[k : k + 1], sin[k : k + 1]))
    return real_idft(out)


def columns_half(x, t):
    y = left(t["td"], x)
    cos, sin = t["twx"][0], t["twx"][1]
    out = []
    for g in range(x.shape[1] // 128):
        part = y[:, 128 * g : 128 * g + 128]
        out.append(turn(part[:half_rows], part[half_rows:], cos, sin))
    return out


def columns_back(parts, t):
    cos, sin = t["twx"][0], t["twx"][1]
    cols = []
    for re, im in parts:
        br, bi = turn_back(re, im, cos, sin)
        cols.append(cat([br, bi], 0))
    return left(t["ti"], cat(cols, 1))


def columns_derivative(x, t):
    parts = columns_half(x, t)
    stacked = cat([cat([re, im], 1) for re, im in parts], 0)
    moved = right(stacked, t["squares"][MX])
    slope = unit * lax.broadcasted_iota(jnp.int32, (half_rows, 128), 0).astype(f32)
    out = []
    for g, (re, im) in enumerate(parts):
        rows = slice(half_rows * g, half_rows * (g + 1))
        out.append((moved[rows, :128] - slope * im, moved[rows, 128:] + slope * re))
    return columns_back(out, t)


def columns_spectrum(x, t):
    parts = columns_half(x, t)
    stacked = cat([cat([re, im], 1) for re, im in parts], 0)
    z = right(stacked, t["squares"][WX])
    row = lax.broadcasted_iota(jnp.int32, (8, 128), 0)
    lane = lax.broadcasted_iota(jnp.int32, (8, 128), 1)
    slot = (row == 0) & (lane >= 64) & (lane < 72)
    out = []
    for g in range(len(parts)):
        base = half_rows * g
        z0, z1 = z[base : base + half_rows, :128], z[base : base + half_rows, 128:]
        top0 = jnp.where(slot, roll(z1[:8], 64), z0[:8])
        top1 = jnp.where(row == 0, z0[64:72], z1[:8])
        out.append((cat([top0, z0[8:64]], 0), cat([top1, z1[8:64]], 0)))
    return out


def columns_field(blocks, t):
    row = lax.broadcasted_iota(jnp.int32, (8, 128), 0)
    lane = lax.broadcasted_iota(jnp.int32, (8, 128), 1)
    first = jnp.where(lane < 8, 1.0, jnp.where((lane >= 64) & (lane < 72), 0.0, 2.0))
    stacked = []
    for x0, x1 in blocks:
        top0 = jnp.where(row == 0, first * x0[:8], x0[:8])
        kept = jnp.where(lane < 8, roll(x0[:8], 64), 0.0)
        top1 = jnp.where(row == 0, kept, x1[:8])
        last0 = jnp.where(row == 0, 2.0 * x1[:8], 0.0)
        stacked.append(
            cat(
                [
                    cat([top0, x0[8:], last0], 0),
                    cat([top1, x1[8:], jnp.zeros_like(last0)], 0),
                ],
                1,
            )
        )
    z = right(cat(stacked, 0), t["squares"][WXI])
    parts = []
    for g in range(len(blocks)):
        rows = slice(half_rows * g, half_rows * (g + 1))
        parts.append((z[rows, :128], z[rows, 128:]))
    return columns_back(parts, t)


def waves_forward(x, t):
    blocks = x.shape[0] // 128
    cos, sin = t["twy"][0], t["twy"][1]
    halves = split(x)
    lanes = []
    for table in (WYA, WYB):
        y = product(halves, (t["squares"][table][0], t["squares"][table][1]))
        for b in range(blocks):
            rows = slice(128 * b, 128 * b + 128)
            re, im = turn(y[rows, :128], y[rows, 128:], cos, sin)
            lanes.append(cat([re, im], 0))
    z = left(t["squares"][TY], cat(lanes, 1))
    out = []
    for b in range(blocks):
        for origin in range(2):
            at = 128 * (origin * blocks + b)
            out.append((z[:128, at : at + 128], z[128:, at : at + 128]))
    return out


def waves_back(values, t):
    cos, sin = t["twy"][0], t["twy"][1]
    z = left(t["squares"][TYI], cat([cat([re, im], 0) for re, im in values], 1))
    rows = []
    for v in range(len(values)):
        part = z[:, 128 * v : 128 * v + 128]
        rows.append(cat(turn_back(part[:128], part[128:], cos, sin), 1))
    y = right(cat(rows, 0), t["squares"][WYI])
    return [y[128 * v : 128 * v + 128] for v in range(len(values))]


def roll(x, shift):
    return pltpu.roll(x, shift, 1)


def denominators(me):
    lane = lax.broadcasted_iota(jnp.int32, (128, 128), 1)
    row = lax.broadcasted_iota(jnp.int32, (128, 128), 0)
    k = lane // 16
    first = jnp.where(me == 1, 64, me // 2) + 1024 * jnp.where(me == 1, 0, me % 2)
    a = first + 128 * k
    b = lane % 16 + 16 * row
    packed = (k == 0) & (me == 0)

    def square(index):
        wave = unit * jnp.where(index < n // 2, index, index - n).astype(f32)
        return wave * wave

    out = []
    for index in (a, jnp.where(packed, n // 2, a)):
        ksq = square(index) + square(b)
        out.append(1.0 / (1.0 + step * (ksq * ksq - ksq)))
    return out[0], out[1], packed


ROWS = dict(t=2, ug=4, f=4, goal=2, w=2, m=2, n=2, fg=4, qv=4, nx=2)
KEYS = tuple(ROWS)
DIRECT = ("ug", "w", "m", "qv", "f")


def hops(offset):
    return sum((0, 1, 2, 1)[offset >> shift & 3] for shift in (1, 3, 5))


FAR_FIRST = sorted(range(peers - 1, 0, -1), key=lambda offset: -hops(offset))


RECEIVED = tuple(key for key in KEYS if key not in ("qv", "nx"))


def kernel(*refs):
    fields_hbm = refs[:3]
    tables_hbm = refs[3 : 3 + len(NAMES)]
    refs = refs[3 + len(NAMES) :]
    objective_ref, slope_ref, fgrad_ref = refs[:3]
    recv = dict(zip(("qv", "nx"), refs[3:5]))
    refs = refs[5:]
    u_ref, t_ref, f_ref = refs[:3]
    refs = refs[3:]
    tables = dict(zip(NAMES, refs[: len(NAMES)]))
    refs = refs[len(NAMES) :]
    send = dict(zip(KEYS, refs[: len(KEYS)]))
    refs = refs[len(KEYS) :]
    recv.update(zip(RECEIVED, refs[: len(RECEIVED)]))
    refs = refs[len(RECEIVED) :]
    part_ref, mid_ref, near_ref, far_ref, g1_ref, g2_ref, forced_ref, goal_ref = refs[:8]
    table_sem, send_sem, recv_sem, own_sem = refs[8:]

    me = lax.axis_index("px") * 8 + lax.axis_index("py")
    barrier = pltpu.get_barrier_semaphore()

    def greet(i, carry):
        d = jnp.bitwise_xor(me, peers - i)
        pl.semaphore_signal(barrier, inc=1, device_id=d, device_id_type=LOGICAL)
        return carry

    lax.fori_loop(1, peers, greet, 0, unroll=4)
    loads = [
        pltpu.make_async_copy(src, dst, table_sem.at[i])
        for i, (src, dst) in enumerate(
            zip(fields_hbm + tables_hbm, [u_ref, t_ref, f_ref] + [tables[k] for k in NAMES])
        )
    ]
    for load in loads:
        load.start()

    def flat(ref):
        return ref.reshape(ref.shape[0] * ref.shape[1], 128)

    def put(key, row, value):
        flat(send[key])[pl.ds(row, peers, ROWS[key]), :] = value

    def get(key, row, count=peers, stride=None):
        return flat(recv[key])[pl.ds(row, count, stride or ROWS[key]), :]

    def start(key):
        i = KEYS.index(key)
        src, dst = send[key], recv[key]
        pltpu.make_async_copy(src.at[me], dst.at[me], own_sem.at[i]).start()

        def one(offset):
            d = jnp.bitwise_xor(me, offset)
            pltpu.make_async_remote_copy(
                src.at[d], dst.at[me], send_sem.at[i], recv_sem.at[i],
                device_id=d, device_id_type=LOGICAL,
            ).start()

        if key in DIRECT:
            for offset in FAR_FIRST:
                one(offset)
        else:
            lax.fori_loop(1, peers, lambda j, c: (one(peers - j), c)[1], 0, unroll=4)

    def whole(key):
        i = KEYS.index(key)
        span = pl.ds(0, peers - 1)
        return pltpu.make_async_remote_copy(
            send[key].at[span], recv[key].at[span], send_sem.at[i], recv_sem.at[i],
            device_id=0, device_id_type=LOGICAL,
        )

    def arrive(key):
        i = KEYS.index(key)
        pltpu.make_async_copy(send[key].at[me], recv[key].at[me], own_sem.at[i]).wait()
        whole(key).wait_recv()

    group, member = jnp.bitwise_and(me, 7), lax.shift_right_logical(me, 3)
    near, far = len(KEYS), len(KEYS) + 1

    def tell(src, dst, sem, offsets):
        for offset in offsets:
            pltpu.make_async_remote_copy(
                src, dst, send_sem.at[sem], recv_sem.at[sem],
                device_id=jnp.bitwise_xor(me, offset), device_id_type=LOGICAL,
            ).start()

    def told(ref, sem):
        others = ref.at[pl.ds(0, ref.shape[0] - 1)]
        return pltpu.make_async_remote_copy(
            others, others, send_sem.at[sem], recv_sem.at[sem],
            device_id=0, device_id_type=LOGICAL,
        )

    def tiles_of(ref):
        return [ref[:, 128 * i : 128 * i + 128] for i in range(16)]

    def put_field(key, row, tiles):
        for g in range(2):
            put(key, row + g, cat(tiles[8 * g : 8 * g + 8], 0).T)

    def get_tiles(key):
        out = []
        for g in range(2):
            block = get(key, g).T
            out += [block[16 * i : 16 * i + 16] for i in range(8)]
        return out

    for load in loads:
        load.wait()
    t = tables
    u_tiles = tiles_of(u_ref)
    put_field("ug", 0, u_tiles)
    put_field("ug", 2, rows_derivative(u_tiles, t))
    put_field("t", 0, tiles_of(t_ref))
    for c in range(2):
        for which in range(2):
            sides = []
            for h in range(2):
                order = range(8) if which == 0 else range(7, -1, -1)
                sides.append(
                    cat([f_ref[c, :, 128 * (8 * h + k) : 128 * (8 * h + k) + 128] for k in order], 0)
                )
            high, low = split(cat(sides, 1))
            dims = (((1,), (1,)), ((), ()))
            place = t["places"][which]
            moved = lax.dot_general(place, high, dims, preferred_element_type=f32)
            moved = moved + lax.dot_general(place, low, dims, preferred_element_type=f32)
            put("f", 2 * which + c, moved)
    pl.semaphore_wait(barrier, peers - 1)
    start("t")
    start("ug")
    start("f")
    r_re, r_im, packed = denominators(me)

    def put_spectrum(key, field):
        for g, blocks in enumerate(columns_spectrum(field, t)):
            for h in range(2):
                flat(send[key])[pl.ds(2 * h + g, 64, 4), :] = blocks[h]

    arrive("t")
    put_spectrum("goal", cat([get("t", 0), get("t", 1)], 1))
    start("goal")
    arrive("ug")
    u = cat([get("ug", 0), get("ug", 1)], 1)
    g2 = cat([get("ug", 2), get("ug", 3)], 1)
    g1 = columns_derivative(u, t)
    g1_ref[...] = g1
    g2_ref[...] = g2
    put_spectrum("w", u + (-0.5 * step) * (g1 * g1 + g2 * g2))
    start("w")

    arrive("f")
    own = (get("f", 0), get("f", 1))
    mirror = tuple(jnp.where(me == 0, roll(get("f", 2 + c), 16), get("f", 2 + c)) for c in range(2))
    here, there = waves_back([own, mirror], t)
    lane = lax.broadcasted_iota(jnp.int32, (128, 128), 1)
    column = lane % 64 // 8
    special = (column == 0) & (me == 0)
    for g in range(2):
        a = here[:, 128 * g : 128 * g + 128]
        b = there[:, 128 * g : 128 * g + 128]
        even = 0.5 * jnp.where(lane < 64, a + b, a - b)
        single = jnp.where(lane < 64, a, roll(b, 64))
        forced_ref[:, 128 * g : 128 * g + 128] = step * jnp.where(special, single, even)

    arrive("goal")
    for i, (re, im) in enumerate(waves_forward(cat([get("goal", 0), get("goal", 1)], 1), t)):
        goal_ref[2 * i] = re
        goal_ref[2 * i + 1] = im
    arrive("w")
    w = cat([get("w", 0), get("w", 1)], 1) + forced_ref[...]
    z_re, z_im = waves_forward(w, t)
    t_re, t_im = (goal_ref[0], goal_ref[1]), (goal_ref[2], goal_ref[3])
    next_re = tuple(r_re * z for z in z_re)
    next_im = tuple(r_im * z for z in z_im)
    miss_re = tuple(a - b for a, b in zip(next_re, t_re))
    miss_im = tuple(a - b for a, b in zip(next_im, t_im))
    c_re = tuple((step * r_re) * v for v in miss_re)
    c_im = tuple((step * r_im) * v for v in miss_im)
    join = lambda x, y: (x[0] - y[1], x[1] + y[0])
    part = lambda x, y: (x[0] + y[1], x[1] - y[0])
    coef = join(c_re, c_im)
    (m_out,) = waves_back([coef], t)
    for g in range(2):
        put("m", g, m_out[:, 128 * g : 128 * g + 128])
    start("m")
    (n_out,) = waves_back([join(next_re, next_im)], t)
    for g in range(2):
        put("n", g, n_out[:, 128 * g : 128 * g + 128])
    start("n")
    other = part(c_re, c_im)
    for c in range(2):
        put("fg", c, jnp.where(packed, c_re[c], coef[c]))
        back = jnp.where(packed, c_im[c], other[c])
        put("fg", 2 + c, jnp.where(me == 0, roll(back, 112), back))
    start("fg")
    miss = join(miss_re, miss_im)
    total = jnp.where(packed, 1.0, 2.0) * (miss[0] * miss[0] + miss[1] * miss[1])
    part_ref[...] = jnp.sum(total, axis=0, keepdims=True)
    near_ref[group] = part_ref[...]
    tell(part_ref, near_ref.at[group], near, [j for j in range(1, 8)])

    def blocks_of(key):
        return [
            tuple(get(key, 2 * h + g, 64, 4) for h in range(2))
            for g in range(2)
        ]

    arrive("m")
    m = columns_field(blocks_of("m"), t)
    q2 = m * g2_ref[...]
    v = 4.0 * m + columns_derivative(m * g1_ref[...], t)
    for g in range(2):
        put("qv", g, q2[:, 128 * g : 128 * g + 128])
        put("qv", 2 + g, v[:, 128 * g : 128 * g + 128])
    start("qv")
    told(near_ref, near).wait_recv()
    mid_ref[...] = jnp.sum(flat(near_ref)[...], axis=0, keepdims=True)
    far_ref[member] = mid_ref[...]
    tell(mid_ref, far_ref.at[member], far, [8 * j for j in range(1, 16)])
    arrive("n")
    stepped = columns_field(blocks_of("n"), t)
    for g in range(2):
        put("nx", g, stepped[:, 128 * g : 128 * g + 128])
    start("nx")

    arrive("fg")
    sides = []
    for which in range(2):
        block = cat([get("fg", 2 * which), get("fg", 2 * which + 1)], 1)
        high, low = split(block)
        place = t["places_t"][which]
        sides.append(dot(place, high) + dot(place, low))
    for h in range(2):
        for c in range(2):
            a = sides[0][128 * h : 128 * h + 128, 128 * c : 128 * c + 128].T
            b = sides[1][128 * h : 128 * h + 128, 128 * c : 128 * c + 128].T
            for k in range(8):
                at = 128 * (8 * h + k)
                fgrad_ref[c, :, at : at + 128] = (
                    a[16 * k : 16 * k + 16] + b[16 * (7 - k) : 16 * (7 - k) + 16]
                )
    told(far_ref, far).wait_recv()
    sums = jnp.sum(flat(far_ref)[...], axis=0, keepdims=True)
    objective_ref[...] = (0.5 / (n * n)) * jnp.sum(sums, axis=1, keepdims=True)
    arrive("qv")
    for i, tile in enumerate(rows_derivative(get_tiles("qv"), t)):
        slope_ref[:, 128 * i : 128 * i + 128] = tile
    arrive("nx")
    for key in KEYS:
        whole(key).wait_send()
    told(near_ref, near).wait_send()
    told(far_ref, far).wait_send()


def finish(
    total_ref, slope_ref, fgrad_ref, v_ref, nx_ref,
    objective_out, grad_out, next_out, fgrad_out, grad, nexts, sems,
):
    objective_out[...] = total_ref[...]
    copies = [
        pltpu.make_async_copy(src, dst, sems.at[i])
        for i, (src, dst) in enumerate(
            ((fgrad_ref, fgrad_out), (grad, grad_out), (nexts, next_out))
        )
    ]
    copies[0].start()
    for ref, out, i, rows, first in ((v_ref, grad, 1, 4, 2), (nx_ref, nexts, 2, 2, 0)):
        for g in range(2):
            block = ref.reshape(rows * peers, 128)[pl.ds(first + g, peers, rows), :].T
            for k in range(8):
                at = 128 * (8 * g + k)
                tile = block[16 * k : 16 * k + 16]
                if i == 1:
                    tile = tile + slope_ref[:, at : at + 128]
                out[:, at : at + 128] = tile
        copies[i].start()
    for copy in copies:
        copy.wait()


def per_device(initial_field, target_field, forcing):
    built = build_tables()
    constants = [jnp.asarray(built[name]) for name in NAMES]
    vmem = pl.BlockSpec(memory_space=pltpu.VMEM)
    hbm = pl.BlockSpec(memory_space=pltpu.HBM)
    message = lambda key: pltpu.VMEM((peers, ROWS[key], 128), f32)
    operands = tuple(
        pltpu.with_memory_space_constraint(x, pltpu.HBM)
        for x in (initial_field[0], target_field[0], forcing, *constants)
    )
    field = jax.ShapeDtypeStruct((16, n), f32)
    both = jax.ShapeDtypeStruct((2, 16, n), f32)
    landing = [jax.ShapeDtypeStruct((peers, ROWS[key], 128), f32) for key in ("qv", "nx")]
    total, slope, forcing_rows, v, nx = pl.pallas_call(
        kernel,
        out_shape=(jax.ShapeDtypeStruct((1, 1), f32), field, both, *landing),
        in_specs=[hbm] * len(operands),
        out_specs=(vmem,) * 5,
        scratch_shapes=[pltpu.VMEM(x.shape, x.dtype) for x in operands]
        + [message(key) for key in KEYS]
        + [message(key) for key in RECEIVED]
        + [
            pltpu.VMEM((1, 128), f32),
            pltpu.VMEM((1, 128), f32),
            pltpu.VMEM((8, 1, 128), f32),
            pltpu.VMEM((16, 1, 128), f32),
            pltpu.VMEM((128, 256), f32),
            pltpu.VMEM((128, 256), f32),
            pltpu.VMEM((128, 256), f32),
            pltpu.VMEM((4, 128, 128), f32),
            pltpu.SemaphoreType.DMA((len(operands),)),
            pltpu.SemaphoreType.DMA((len(KEYS) + 2,)),
            pltpu.SemaphoreType.DMA((len(KEYS) + 2,)),
            pltpu.SemaphoreType.DMA((len(KEYS),)),
        ],
        compiler_params=pltpu.CompilerParams(
            collective_id=0, has_side_effects=True, vmem_limit_bytes=32 * 1024 * 1024
        ),
    )(*operands)
    objective, field_grad, next_field, forcing_grad = pl.pallas_call(
        finish,
        out_shape=(jax.ShapeDtypeStruct((1, 1), f32), field, field, both),
        in_specs=[vmem] * 5,
        out_specs=(vmem,) + (hbm,) * 3,
        scratch_shapes=[
            pltpu.VMEM((16, n), f32),
            pltpu.VMEM((16, n), f32),
            pltpu.SemaphoreType.DMA((3,)),
        ],
        compiler_params=pltpu.CompilerParams(vmem_limit_bytes=8 * 1024 * 1024),
    )(total, slope, forcing_rows, v, nx)
    return next_field[None], objective.reshape(()), field_grad[None], forcing_grad


def solution(mesh):
    spec = P(None, ("px", "py"), None)
    return jax.shard_map(
        per_device,
        mesh=mesh,
        in_specs=(spec, spec, spec),
        out_specs=(spec, P(), spec, spec),
        check_vma=False,
    )
```

```python
import math

import jax
import jax.numpy as jnp
import numpy as np
from jax import lax
from jax.experimental import pallas as pl
from jax.experimental.pallas import tpu as pltpu
from jax.sharding import PartitionSpec as P

LOGICAL = pl.DeviceIdType.LOGICAL
f32 = jnp.float32
bf16 = jnp.bfloat16

n = 2048
peers = 128
step = 0.25
unit = 4.0 / n
half_rows = 72


def cplx(table):
    return np.block([[table.real, table.imag], [-table.imag, table.real]])


def signed(count, index):
    return np.where(index < count // 2, index, index - count)


def build_tables():
    s = np.arange(128)
    a1 = np.arange(65)
    theta = 2 * np.pi * np.outer(a1, s) / 128
    td = np.zeros((2 * half_rows, 128))
    td[:65] = np.cos(theta)
    td[half_rows : half_rows + 65] = -np.sin(theta)
    weight = np.where((a1 == 0) | (a1 == 64), 1.0, 2.0) / 128
    ti = np.zeros((128, 2 * half_rows))
    ti[:, :65] = (np.cos(theta) * weight[:, None]).T
    ti[:, half_rows : half_rows + 65] = (-np.sin(theta) * weight[:, None]).T

    def derivative(length, factor):
        freq = signed(length, s[:length]).astype(float) * factor
        inner = np.where(s[:length] == length // 2, 0.0, freq)
        gap = np.subtract.outer(s[:length], s[:length])
        waves = np.exp(2j * np.pi * gap[:, :, None] * s[:length] / length)
        smooth = (waves * (1j * inner)).sum(-1).real / length
        nyquist = freq[length // 2] * (-1.0) ** gap / length
        return (smooth + 1j * nyquist).T

    root = 1.0 / math.sqrt(n)
    mx = cplx(np.kron(np.eye(8), derivative(16, unit * 128)))
    my = cplx(derivative(128, unit * 16) / 16)

    w16 = np.exp(-2j * np.pi * np.outer(s[:16], s[:16]) / 16)
    eye8 = np.eye(8)
    forward = w16.reshape(16, 2, 8)
    parts = np.zeros((2, 8, 16, 2, 2, 8, 8))
    for y in range(8):
        parts[0, y, :, :, 0, :, y] = forward.real
        parts[0, y, :, :, 1, :, y] = forward.imag
        parts[1, y, :, :, 0, :, y] = -forward.imag
        parts[1, y, :, :, 1, :, y] = forward.real
    wx = parts.reshape(256, 256) * root
    back = w16.conj().T.reshape(2, 8, 16)
    parts = np.zeros((2, 2, 8, 8, 2, 8, 16))
    for y in range(8):
        parts[:, 0, :, y, 0, y, :] = back.real
        parts[:, 0, :, y, 1, y, :] = back.imag
        parts[:, 1, :, y, 0, y, :] = -back.imag
        parts[:, 1, :, y, 1, y, :] = back.real
    wxi = parts.reshape(256, 256) * (128 * root)
    forward = w16.reshape(2, 8, 16)
    parts = np.zeros((2, 2, 8, 8, 2, 2, 8, 16))
    for k in range(8):
        for c in range(2):
            parts[:, c, k, :, c, 0, k, :] = forward.real
            parts[:, c, k, :, c, 1, k, :] = forward.imag
    wy = parts.reshape(256, 512)
    back = w16.conj().T.reshape(16, 2, 8)
    parts = np.zeros((2, 8, 16, 2, 2, 8, 8))
    for k in range(8):
        parts[0, k, :, :, 0, k, :] = back.real
        parts[0, k, :, :, 1, k, :] = back.imag
        parts[1, k, :, :, 0, k, :] = -back.imag
        parts[1, k, :, :, 1, k, :] = back.real
    wyi = parts.reshape(256, 256)
    f128 = np.exp(-2j * np.pi * np.outer(s, s) / 128) * root
    ty = cplx(f128).T
    squares = np.stack([mx, my, wx, wxi, wy[:, :256], wy[:, 256:], wyi, ty])

    own = np.zeros((128, 2, 128))
    mirror = np.zeros((128, 2, 128))
    for e in range(128):
        h, a = e % 2, e // 2
        if e == 0:
            own[e, 0, 0] = mirror[e, 1, 0] = 1
        elif e == 1:
            own[e, 0, 64] = mirror[e, 1, 64] = 1
        else:
            own[e, h, a] = mirror[e, 1 - h, 128 - a] = 1
    places = np.stack([own.reshape(128, 256), mirror.reshape(128, 256)])

    row = np.arange(half_rows)[:, None]
    lane = np.arange(128)[None, :]
    twx = 2 * np.pi * row * (lane % 16) / n
    twy = 2 * np.pi * np.arange(128)[:, None] * (lane % 16) / n
    twr = 2 * np.pi * np.arange(16)[:, None] * lane / n
    both = lambda t: np.stack([np.cos(t), np.sin(t)]).astype(np.float32)

    def halves(t):
        high = t.astype(np.float32).astype(bf16)
        low = (t - high.astype(np.float64)).astype(np.float32).astype(bf16)
        return high, low

    return dict(
        squares=np.stack(halves(squares), axis=1),
        td=np.stack(halves(td)),
        ti=np.stack(halves(ti)),
        places=places.astype(np.float32).astype(bf16),
        places_t=places.transpose(0, 2, 1).astype(np.float32).astype(bf16),
        twx=both(twx),
        twy=both(twy),
        twr=both(twr),
    )


MX, MY, WX, WXI, WYA, WYB, WYI, TY = range(8)
NAMES = ("squares", "td", "ti", "places", "places_t", "twx", "twy", "twr")


def split(x):
    high = x.astype(bf16)
    return high, (x - high.astype(f32)).astype(bf16)


def dot(a, b):
    return jnp.dot(a, b, preferred_element_type=f32)


def product(a, b):
    return dot(a[0], b[0]) + (dot(a[0], b[1]) + dot(a[1], b[0]))


def left(table, x):
    return product((table[0], table[1]), split(x))


def right(x, table):
    return product(split(x), (table[0], table[1]))


def cat(parts, axis):
    return jnp.concatenate(parts, axis=axis)


def turn(re, im, cos, sin):
    return re * cos + im * sin, im * cos - re * sin


def turn_back(re, im, cos, sin):
    return re * cos - im * sin, im * cos + re * sin


def real_dft(values):
    count = len(values)
    if count == 2:
        return [(values[0] + values[1], None), (values[0] - values[1], None)]
    even, odd = real_dft(values[0::2]), real_dft(values[1::2])
    quarter = count // 4
    out = [None] * (count // 2 + 1)
    for k in range(quarter + 1):
        (er, ei), (tr, ti) = even[k], odd[k]
        if k == quarter:
            out[k] = (er, -tr)
            continue
        if k > 0:
            c, s = math.cos(2 * math.pi * k / count), math.sin(2 * math.pi * k / count)
            tr, ti = (tr * c + ti * s, ti * c - tr * s) if ti is not None else (tr * c, tr * -s)
        if k == 0:
            out[0], out[count // 2] = (er + tr, None), (er - tr, None)
        else:
            ei = 0.0 if ei is None else ei
            out[k] = (er + tr, ei + ti)
            out[count // 2 - k] = (er - tr, ti - ei)
    return out


def real_idft(spectrum):
    count = 2 * (len(spectrum) - 1)
    if count == 2:
        return [spectrum[0][0] + spectrum[1][0], spectrum[0][0] - spectrum[1][0]]
    quarter = count // 4
    even, odd = [], []
    for k in range(quarter + 1):
        re, im = spectrum[k]
        if k == 0:
            other = spectrum[count // 2][0]
            even.append((re + other, None))
            odd.append((re - other, None))
        elif k == quarter:
            even.append((2.0 * re, None))
            odd.append((-2.0 * im, None))
        else:
            hr, hi = spectrum[count // 2 - k]
            even.append((re + hr, im - hi))
            dr, di = re - hr, im + hi
            c, s = math.cos(2 * math.pi * k / count), math.sin(2 * math.pi * k / count)
            odd.append((dr * c - di * s, dr * s + di * c))
    xs, ys = real_idft(even), real_idft(odd)
    return [v for pair in zip(xs, ys) for v in pair]


def rows_derivative(tiles, t):
    cos, sin = t["twr"][0], t["twr"][1]
    turned = []
    for k, (re, im) in enumerate(real_dft(tiles)):
        c, s = cos[k : k + 1], sin[k : k + 1]
        if k == 0:
            turned.append((re, jnp.zeros_like(re)))
        elif im is None:
            turned.append((re * c, -re * s))
        else:
            turned.append(turn(re, im, c, s))
    re_rows = cat([v[0] for v in turned], 0)
    im_rows = cat([v[1] for v in turned], 0)
    moved = right(cat([re_rows, im_rows], 1), t["squares"][MY])
    out = []
    for k, (re, im) in enumerate(turned):
        mr = moved[16 * k : 16 * k + 16, :128] - (unit / 16 * k) * im
        mi = moved[16 * k : 16 * k + 16, 128:] + (unit / 16 * k) * re
        out.append(turn_back(mr, mi, cos[k : k + 1], sin[k : k + 1]))
    return real_idft(out)


def columns_half(x, t):
    y = left(t["td"], x)
    cos, sin = t["twx"][0], t["twx"][1]
    out = []
    for g in range(x.shape[1] // 128):
        part = y[:, 128 * g : 128 * g + 128]
        out.append(turn(part[:half_rows], part[half_rows:], cos, sin))
    return out


def columns_back(parts, t):
    cos, sin = t["twx"][0], t["twx"][1]
    cols = []
    for re, im in parts:
        br, bi = turn_back(re, im, cos, sin)
        cols.append(cat([br, bi], 0))
    return left(t["ti"], cat(cols, 1))


def columns_derivative(x, t):
    parts = columns_half(x, t)
    stacked = cat([cat([re, im], 1) for re, im in parts], 0)
    moved = right(stacked, t["squares"][MX])
    slope = unit * lax.broadcasted_iota(jnp.int32, (half_rows, 128), 0).astype(f32)
    out = []
    for g, (re, im) in enumerate(parts):
        rows = slice(half_rows * g, half_rows * (g + 1))
        out.append((moved[rows, :128] - slope * im, moved[rows, 128:] + slope * re))
    return columns_back(out, t)


def columns_spectrum(x, t):
    parts = columns_half(x, t)
    stacked = cat([cat([re, im], 1) for re, im in parts], 0)
    z = right(stacked, t["squares"][WX])
    row = lax.broadcasted_iota(jnp.int32, (8, 128), 0)
    lane = lax.broadcasted_iota(jnp.int32, (8, 128), 1)
    slot = (row == 0) & (lane >= 64) & (lane < 72)
    out = []
    for g in range(len(parts)):
        base = half_rows * g
        z0, z1 = z[base : base + half_rows, :128], z[base : base + half_rows, 128:]
        top0 = jnp.where(slot, roll(z1[:8], 64), z0[:8])
        top1 = jnp.where(row == 0, z0[64:72], z1[:8])
        out.append((cat([top0, z0[8:64]], 0), cat([top1, z1[8:64]], 0)))
    return out


def columns_field(blocks, t):
    row = lax.broadcasted_iota(jnp.int32, (8, 128), 0)
    lane = lax.broadcasted_iota(jnp.int32, (8, 128), 1)
    first = jnp.where(lane < 8, 1.0, jnp.where((lane >= 64) & (lane < 72), 0.0, 2.0))
    stacked = []
    for x0, x1 in blocks:
        top0 = jnp.where(row == 0, first * x0[:8], x0[:8])
        kept = jnp.where(lane < 8, roll(x0[:8], 64), 0.0)
        top1 = jnp.where(row == 0, kept, x1[:8])
        last0 = jnp.where(row == 0, 2.0 * x1[:8], 0.0)
        stacked.append(
            cat(
                [
                    cat([top0, x0[8:], last0], 0),
                    cat([top1, x1[8:], jnp.zeros_like(last0)], 0),
                ],
                1,
            )
        )
    z = right(cat(stacked, 0), t["squares"][WXI])
    parts = []
    for g in range(len(blocks)):
        rows = slice(half_rows * g, half_rows * (g + 1))
        parts.append((z[rows, :128], z[rows, 128:]))
    return columns_back(parts, t)


def waves_forward(x, t):
    blocks = x.shape[0] // 128
    cos, sin = t["twy"][0], t["twy"][1]
    halves = split(x)
    lanes = []
    for table in (WYA, WYB):
        y = product(halves, (t["squares"][table][0], t["squares"][table][1]))
        for b in range(blocks):
            rows = slice(128 * b, 128 * b + 128)
            re, im = turn(y[rows, :128], y[rows, 128:], cos, sin)
            lanes.append(cat([re, im], 0))
    z = left(t["squares"][TY], cat(lanes, 1))
    out = []
    for b in range(blocks):
        for origin in range(2):
            at = 128 * (origin * blocks + b)
            out.append((z[:128, at : at + 128], z[128:, at : at + 128]))
    return out


def waves_back(values, t):
    cos, sin = t["twy"][0], t["twy"][1]
    z = left(t["inverse"], cat([cat([re, im], 0) for re, im in values], 1))
    rows = []
    for v in range(len(values)):
        part = z[:, 128 * v : 128 * v + 128]
        rows.append(cat(turn_back(part[:128], part[128:], cos, sin), 1))
    y = right(cat(rows, 0), t["squares"][WYI])
    return [y[128 * v : 128 * v + 128] for v in range(len(values))]


def roll(x, shift):
    return pltpu.roll(x, shift, 1)


def denominators(me):
    lane = lax.broadcasted_iota(jnp.int32, (128, 128), 1)
    row = lax.broadcasted_iota(jnp.int32, (128, 128), 0)
    k = lane // 16
    first = jnp.where(me == 1, 64, me // 2) + 1024 * jnp.where(me == 1, 0, me % 2)
    a = first + 128 * k
    b = lane % 16 + 16 * row
    packed = (k == 0) & (me == 0)

    def square(index):
        wave = unit * jnp.where(index < n // 2, index, index - n).astype(f32)
        return wave * wave

    out = []
    for index in (a, jnp.where(packed, n // 2, a)):
        ksq = square(index) + square(b)
        out.append(1.0 / (1.0 + step * (ksq * ksq - ksq)))
    return out[0], out[1], packed


ROWS = dict(t=2, ug=4, f=4, goal=2, w=2, m=2, n=2, fg=4, qv=4, nx=2)
KEYS = tuple(ROWS)
DIRECT = ("ug", "w", "m", "qv", "f", "fg", "nx")


def hops(offset):
    return sum((0, 1, 2, 1)[offset >> shift & 3] for shift in (1, 3, 5))


FAR_FIRST = sorted(range(peers - 1, 0, -1), key=lambda offset: -hops(offset))


RECEIVED = tuple(key for key in KEYS if key != "nx")


def kernel(*refs):
    fields_hbm = refs[:3]
    tables_hbm = refs[3 : 3 + len(NAMES)]
    refs = refs[3 + len(NAMES) :]
    objective_ref, grad_ref, fgrad_ref = refs[:3]
    recv = dict(nx=refs[3])
    refs = refs[4:]
    u_ref, t_ref, f_ref = refs[:3]
    refs = refs[3:]
    tables = dict(zip(NAMES, refs[: len(NAMES)]))
    refs = refs[len(NAMES) :]
    send = dict(zip(KEYS, refs[: len(KEYS)]))
    refs = refs[len(KEYS) :]
    recv.update(zip(RECEIVED, refs[: len(RECEIVED)]))
    refs = refs[len(RECEIVED) :]
    part_ref, mid_ref, near_ref, far_ref, g1_ref, g2_ref, forced_ref, goal_ref, inverse_ref = refs[:9]
    table_sem, send_sem, recv_sem, own_sem = refs[9:]

    me = lax.axis_index("px") * 8 + lax.axis_index("py")
    barrier = pltpu.get_barrier_semaphore()

    def greet(i, carry):
        d = jnp.bitwise_xor(me, peers - i)
        pl.semaphore_signal(barrier, inc=1, device_id=d, device_id_type=LOGICAL)
        return carry

    lax.fori_loop(1, peers, greet, 0, unroll=4)
    loads = [
        pltpu.make_async_copy(src, dst, table_sem.at[i])
        for i, (src, dst) in enumerate(
            zip(fields_hbm + tables_hbm, [u_ref, t_ref, f_ref] + [tables[k] for k in NAMES])
        )
    ]
    for load in loads:
        load.start()

    def flat(ref):
        return ref.reshape(ref.shape[0] * ref.shape[1], 128)

    def put(key, row, value):
        flat(send[key])[pl.ds(row, peers, ROWS[key]), :] = value

    def get(key, row, count=peers, stride=None):
        return flat(recv[key])[pl.ds(row, count, stride or ROWS[key]), :]

    def start(key):
        i = KEYS.index(key)
        src, dst = send[key], recv[key]
        pltpu.make_async_copy(src.at[me], dst.at[me], own_sem.at[i]).start()

        def one(offset):
            d = jnp.bitwise_xor(me, offset)
            pltpu.make_async_remote_copy(
                src.at[d], dst.at[me], send_sem.at[i], recv_sem.at[i],
                device_id=d, device_id_type=LOGICAL,
            ).start()

        if key in DIRECT:
            for offset in FAR_FIRST:
                one(offset)
        else:
            lax.fori_loop(1, peers, lambda j, c: (one(peers - j), c)[1], 0, unroll=4)

    def whole(key):
        i = KEYS.index(key)
        span = pl.ds(0, peers - 1)
        return pltpu.make_async_remote_copy(
            send[key].at[span], recv[key].at[span], send_sem.at[i], recv_sem.at[i],
            device_id=0, device_id_type=LOGICAL,
        )

    def arrive(key):
        i = KEYS.index(key)
        pltpu.make_async_copy(send[key].at[me], recv[key].at[me], own_sem.at[i]).wait()
        whole(key).wait_recv()

    group, member = jnp.bitwise_and(me, 7), lax.shift_right_logical(me, 3)
    near, far = len(KEYS), len(KEYS) + 1

    def tell(src, dst, sem, offsets):
        for offset in offsets:
            pltpu.make_async_remote_copy(
                src, dst, send_sem.at[sem], recv_sem.at[sem],
                device_id=jnp.bitwise_xor(me, offset), device_id_type=LOGICAL,
            ).start()

    def told(ref, sem):
        others = ref.at[pl.ds(0, ref.shape[0] - 1)]
        return pltpu.make_async_remote_copy(
            others, others, send_sem.at[sem], recv_sem.at[sem],
            device_id=0, device_id_type=LOGICAL,
        )

    def tiles_of(ref):
        return [ref[:, 128 * i : 128 * i + 128] for i in range(16)]

    def put_field(key, row, tiles):
        for g in range(2):
            put(key, row + g, cat(tiles[8 * g : 8 * g + 8], 0).T)

    def get_tiles(key, row=0):
        out = []
        for g in range(2):
            block = get(key, row + g).T
            out += [block[16 * i : 16 * i + 16] for i in range(8)]
        return out

    for load in loads:
        load.wait()
    forward = tables["squares"]
    inverse_ref[...] = forward[TY]
    for half in range(2):
        inverse_ref[half, :128, 128:] = forward[TY, half, 128:, :128]
        inverse_ref[half, 128:, :128] = forward[TY, half, :128, 128:]
    t = dict(tables, inverse=inverse_ref)
    u_tiles = tiles_of(u_ref)
    put_field("ug", 0, u_tiles)
    put_field("ug", 2, rows_derivative(u_tiles, t))
    put_field("t", 0, tiles_of(t_ref))
    for c in range(2):
        for which in range(2):
            sides = []
            for h in range(2):
                order = range(8) if which == 0 else range(7, -1, -1)
                sides.append(
                    cat([f_ref[c, :, 128 * (8 * h + k) : 128 * (8 * h + k) + 128] for k in order], 0)
                )
            high, low = split(cat(sides, 1))
            dims = (((1,), (1,)), ((), ()))
            place = t["places"][which]
            moved = lax.dot_general(place, high, dims, preferred_element_type=f32)
            moved = moved + lax.dot_general(place, low, dims, preferred_element_type=f32)
            put("f", 2 * which + c, moved)
    pl.semaphore_wait(barrier, peers - 1)
    start("t")
    start("ug")
    start("f")
    r_re, r_im, packed = denominators(me)

    def put_spectrum(key, field):
        for g, blocks in enumerate(columns_spectrum(field, t)):
            for h in range(2):
                flat(send[key])[pl.ds(2 * h + g, 64, 4), :] = blocks[h]

    arrive("t")
    put_spectrum("goal", cat([get("t", 0), get("t", 1)], 1))
    start("goal")
    arrive("ug")
    u = cat([get("ug", 0), get("ug", 1)], 1)
    g2 = cat([get("ug", 2), get("ug", 3)], 1)
    g1 = columns_derivative(u, t)
    g1_ref[...] = g1
    g2_ref[...] = g2
    put_spectrum("w", u + (-0.5 * step) * (g1 * g1 + g2 * g2))
    start("w")

    arrive("f")
    own = (get("f", 0), get("f", 1))
    mirror = tuple(jnp.where(me == 0, roll(get("f", 2 + c), 16), get("f", 2 + c)) for c in range(2))
    here, there = waves_back([own, mirror], t)
    lane = lax.broadcasted_iota(jnp.int32, (128, 128), 1)
    column = lane % 64 // 8
    special = (column == 0) & (me == 0)
    for g in range(2):
        a = here[:, 128 * g : 128 * g + 128]
        b = there[:, 128 * g : 128 * g + 128]
        even = 0.5 * jnp.where(lane < 64, a + b, a - b)
        single = jnp.where(lane < 64, a, roll(b, 64))
        forced_ref[:, 128 * g : 128 * g + 128] = step * jnp.where(special, single, even)

    arrive("goal")
    for i, (re, im) in enumerate(waves_forward(cat([get("goal", 0), get("goal", 1)], 1), t)):
        goal_ref[2 * i] = re
        goal_ref[2 * i + 1] = im
    arrive("w")
    w = cat([get("w", 0), get("w", 1)], 1) + forced_ref[...]
    z_re, z_im = waves_forward(w, t)
    t_re, t_im = (goal_ref[0], goal_ref[1]), (goal_ref[2], goal_ref[3])
    next_re = tuple(r_re * z for z in z_re)
    next_im = tuple(r_im * z for z in z_im)
    miss_re = tuple(a - b for a, b in zip(next_re, t_re))
    miss_im = tuple(a - b for a, b in zip(next_im, t_im))
    c_re = tuple((step * r_re) * v for v in miss_re)
    c_im = tuple((step * r_im) * v for v in miss_im)
    join = lambda x, y: (x[0] - y[1], x[1] + y[0])
    part = lambda x, y: (x[0] + y[1], x[1] - y[0])
    coef = join(c_re, c_im)
    (m_out,) = waves_back([coef], t)
    for g in range(2):
        put("m", g, m_out[:, 128 * g : 128 * g + 128])
    start("m")
    (n_out,) = waves_back([join(next_re, next_im)], t)
    for g in range(2):
        put("n", g, n_out[:, 128 * g : 128 * g + 128])
    start("n")
    other = part(c_re, c_im)
    for c in range(2):
        put("fg", c, jnp.where(packed, c_re[c], coef[c]))
        back = jnp.where(packed, c_im[c], other[c])
        put("fg", 2 + c, jnp.where(me == 0, roll(back, 112), back))
    start("fg")
    miss = join(miss_re, miss_im)
    total = jnp.where(packed, 1.0, 2.0) * (miss[0] * miss[0] + miss[1] * miss[1])
    part_ref[...] = jnp.sum(total, axis=0, keepdims=True)
    near_ref[group] = part_ref[...]
    tell(part_ref, near_ref.at[group], near, [j for j in range(1, 8)])

    def blocks_of(key):
        return [
            tuple(get(key, 2 * h + g, 64, 4) for h in range(2))
            for g in range(2)
        ]

    arrive("m")
    m = columns_field(blocks_of("m"), t)
    q2 = m * g2_ref[...]
    v = 4.0 * m + columns_derivative(m * g1_ref[...], t)
    for g in range(2):
        put("qv", g, q2[:, 128 * g : 128 * g + 128])
        put("qv", 2 + g, v[:, 128 * g : 128 * g + 128])
    start("qv")
    told(near_ref, near).wait_recv()
    mid_ref[...] = jnp.sum(flat(near_ref)[...], axis=0, keepdims=True)
    far_ref[member] = mid_ref[...]
    tell(mid_ref, far_ref.at[member], far, [8 * j for j in range(1, 16)])
    arrive("n")
    stepped = columns_field(blocks_of("n"), t)
    for g in range(2):
        put("nx", g, stepped[:, 128 * g : 128 * g + 128])
    start("nx")

    arrive("fg")
    sides = []
    for which in range(2):
        block = cat([get("fg", 2 * which), get("fg", 2 * which + 1)], 1)
        high, low = split(block)
        place = t["places_t"][which]
        sides.append(dot(place, high) + dot(place, low))
    for h in range(2):
        for c in range(2):
            a = sides[0][128 * h : 128 * h + 128, 128 * c : 128 * c + 128].T
            b = sides[1][128 * h : 128 * h + 128, 128 * c : 128 * c + 128].T
            for k in range(8):
                at = 128 * (8 * h + k)
                fgrad_ref[c, :, at : at + 128] = (
                    a[16 * k : 16 * k + 16] + b[16 * (7 - k) : 16 * (7 - k) + 16]
                )
    told(far_ref, far).wait_recv()
    sums = jnp.sum(flat(far_ref)[...], axis=0, keepdims=True)
    objective_ref[...] = (0.5 / (n * n)) * jnp.sum(sums, axis=1, keepdims=True)
    arrive("qv")
    slope = rows_derivative(get_tiles("qv"), t)
    for i, tile in enumerate(get_tiles("qv", 2)):
        grad_ref[:, 128 * i : 128 * i + 128] = tile + slope[i]
    arrive("nx")
    for key in KEYS:
        whole(key).wait_send()
    told(near_ref, near).wait_send()
    told(far_ref, far).wait_send()


def finish(
    total_ref, grad_ref, fgrad_ref, nx_ref,
    objective_out, grad_out, next_out, fgrad_out, nexts, sems,
):
    objective_out[...] = total_ref[...]
    copies = [
        pltpu.make_async_copy(src, dst, sems.at[i])
        for i, (src, dst) in enumerate(
            ((fgrad_ref, fgrad_out), (grad_ref, grad_out), (nexts, next_out))
        )
    ]
    copies[0].start()
    copies[1].start()
    for g in range(2):
        block = nx_ref.reshape(2 * peers, 128)[pl.ds(g, peers, 2), :].T
        for k in range(8):
            at = 128 * (8 * g + k)
            nexts[:, at : at + 128] = block[16 * k : 16 * k + 16]
    copies[2].start()
    for copy in copies:
        copy.wait()


def per_device(initial_field, target_field, forcing):
    built = build_tables()
    constants = [jnp.asarray(built[name]) for name in NAMES]
    vmem = pl.BlockSpec(memory_space=pltpu.VMEM)
    hbm = pl.BlockSpec(memory_space=pltpu.HBM)
    message = lambda key: pltpu.VMEM((peers, ROWS[key], 128), f32)
    operands = tuple(
        pltpu.with_memory_space_constraint(x, pltpu.HBM)
        for x in (initial_field[0], target_field[0], forcing, *constants)
    )
    field = jax.ShapeDtypeStruct((16, n), f32)
    both = jax.ShapeDtypeStruct((2, 16, n), f32)
    landing = jax.ShapeDtypeStruct((peers, ROWS["nx"], 128), f32)
    total, grad_rows, forcing_rows, nx = pl.pallas_call(
        kernel,
        out_shape=(jax.ShapeDtypeStruct((1, 1), f32), field, both, landing),
        in_specs=[hbm] * len(operands),
        out_specs=(vmem,) * 4,
        scratch_shapes=[pltpu.VMEM(x.shape, x.dtype) for x in operands]
        + [message(key) for key in KEYS]
        + [message(key) for key in RECEIVED]
        + [
            pltpu.VMEM((1, 128), f32),
            pltpu.VMEM((1, 128), f32),
            pltpu.VMEM((8, 1, 128), f32),
            pltpu.VMEM((16, 1, 128), f32),
            pltpu.VMEM((128, 256), f32),
            pltpu.VMEM((128, 256), f32),
            pltpu.VMEM((128, 256), f32),
            pltpu.VMEM((4, 128, 128), f32),
            pltpu.VMEM((2, 256, 256), bf16),
            pltpu.SemaphoreType.DMA((len(operands),)),
            pltpu.SemaphoreType.DMA((len(KEYS) + 2,)),
            pltpu.SemaphoreType.DMA((len(KEYS) + 2,)),
            pltpu.SemaphoreType.DMA((len(KEYS),)),
        ],
        compiler_params=pltpu.CompilerParams(
            collective_id=0, has_side_effects=True, vmem_limit_bytes=32 * 1024 * 1024
        ),
    )(*operands)
    objective, field_grad, next_field, forcing_grad = pl.pallas_call(
        finish,
        out_shape=(jax.ShapeDtypeStruct((1, 1), f32), field, field, both),
        in_specs=[vmem] * 4,
        out_specs=(vmem,) + (hbm,) * 3,
        scratch_shapes=[
            pltpu.VMEM((16, n), f32),
            pltpu.SemaphoreType.DMA((3,)),
        ],
        compiler_params=pltpu.CompilerParams(vmem_limit_bytes=8 * 1024 * 1024),
    )(total, grad_rows, forcing_rows, nx)
    return next_field[None], objective.reshape(()), field_grad[None], forcing_grad


def solution(mesh):
    spec = P(None, ("px", "py"), None)
    return jax.shard_map(
        per_device,
        mesh=mesh,
        in_specs=(spec, spec, spec),
        out_specs=(spec, P(), spec, spec),
        check_vma=False,
    )
```
